32 devices in a mesh: dp: 1 (over z), tp: 4 (over y), sp: 8 (over x, core).
Axes of the slice: x: 4, y: 4, z: 1, core: 2. Of those that a mesh axis runs over, the one named last changes fastest.
The devices are a block of a 4x4x8 slice.
Arguments:
- hidden: bfloat16 [32, 4096], P('dp')
- positions: int32 [32], P('dp')
- norm_attn: float32 [4096], replicated
- norm_mlp: float32 [4096], replicated
- w_qkv: bfloat16 [4096, 6144], P(None, 'tp')
- w_out: bfloat16 [4096, 4096], P('tp')
- w_gate_up: bfloat16 [4096, 28672], P(None, 'tp')
- w_down: bfloat16 [14336, 4096], P('tp')
- k_cache: bfloat16 [32, 4096, 8, 128], P('dp', 'sp', 'tp')
- v_cache: bfloat16 [32, 4096, 8, 128], P('dp', 'sp', 'tp')
Outputs:
- output 1: bfloat16 [32, 4096], P('dp')
- output 2: bfloat16 [32, 4096, 8, 128], P('dp', 'sp', 'tp')
- output 3: bfloat16 [32, 4096, 8, 128], P('dp', 'sp', 'tp')
All inputs are finite; a program needn't handle non-finite values.
Results may differ from the reference program's by a relative error of at most 0.00869829.
Values sent between devices are 32-bit elements.
A program may use at most 768 MiB of HBM per device.

```python
import jax
import jax.numpy as jnp
from jax import lax

NUM_SEQS = 32
CACHE_LEN = 4096
TEN_PAR = 4
MODEL_DIM = 4096
NUM_HEADS = 32
KV_HEADS = 8
HEAD_DIM = 128
FFN_DIM = 14336
WINDOW = 2047

GROUP_SIZE = NUM_HEADS // KV_HEADS
QKV_COLS = (NUM_HEADS + 2 * KV_HEADS) * HEAD_DIM
FFN_LOCAL = FFN_DIM // TEN_PAR
ROPE_BASE = 10000.0
NORM_EPS = 1e-5


def rms_norm(values, gain_vec):
    mean_sq = jnp.mean(values * values, axis=-1, keepdims=True)
    return values * lax.rsqrt(mean_sq + NORM_EPS) * gain_vec


def rope_angles(positions):
    inv_freq = ROPE_BASE ** (-jnp.arange(0, HEAD_DIM, 2).astype(jnp.float32) / HEAD_DIM)
    angles = positions.astype(jnp.float32)[:, None] * inv_freq[None, :]
    angles = jnp.concatenate([angles, angles], axis=-1)
    return jnp.cos(angles), jnp.sin(angles)


def rotate_half(values, cos_tab, sin_tab):
    half_dim = values.shape[-1] // 2
    turned = jnp.concatenate([-values[..., half_dim:], values[..., :half_dim]], axis=-1)
    return values * cos_tab + turned * sin_tab


def seq_attention(operands):
    q_rows, k_seq, v_seq, position = operands
    scores = jnp.einsum('kgd,jkd->kgj', q_rows.astype(jnp.float32), k_seq.astype(jnp.float32)) * (HEAD_DIM ** -0.5)
    slot_ids = jnp.arange(CACHE_LEN)
    in_window = (slot_ids <= position) & (slot_ids >= position - WINDOW)
    scores = jnp.where(in_window, scores, -jnp.inf)
    row_max = jnp.max(scores, axis=-1, keepdims=True)
    weights = jnp.exp(scores - row_max)
    weight_sum = jnp.sum(weights, axis=-1)
    acc_sum = jnp.einsum('kgj,jkd->kgd', weights.astype(jnp.bfloat16).astype(jnp.float32), v_seq.astype(jnp.float32))
    return (acc_sum / weight_sum[..., None]).astype(jnp.bfloat16)


def setup_inputs(seed: int = 0, part: int = 0) -> dict:
    base_key = jax.random.key(seed)
    shared_keys = jax.random.split(base_key, 6)
    own_keys = jax.random.split(jax.random.fold_in(base_key, part), 6)
    cache_shape = (NUM_SEQS, CACHE_LEN, KV_HEADS, HEAD_DIM)
    hidden = jax.random.normal(own_keys[0], (NUM_SEQS, MODEL_DIM), jnp.float32).astype(jnp.bfloat16)
    low_pos = WINDOW // 2
    drawn_pos = jax.random.randint(own_keys[1], (NUM_SEQS,), low_pos, CACHE_LEN, jnp.int32)
    row_ids = jnp.arange(NUM_SEQS)
    positions = jnp.where(row_ids == 0, CACHE_LEN - 1, drawn_pos)
    positions = jnp.where(jnp.logical_and(row_ids == NUM_SEQS - 1, NUM_SEQS > 1), low_pos, positions).astype(jnp.int32)
    norm_attn = 1.0 + 0.3 * jax.random.normal(shared_keys[0], (MODEL_DIM,), jnp.float32)
    norm_mlp = 1.0 + 0.3 * jax.random.normal(shared_keys[1], (MODEL_DIM,), jnp.float32)
    w_qkv = (jax.random.normal(shared_keys[2], (MODEL_DIM, QKV_COLS), jnp.float32) * MODEL_DIM ** -0.5).astype(jnp.bfloat16)
    w_out = (jax.random.normal(shared_keys[3], (NUM_HEADS * HEAD_DIM, MODEL_DIM), jnp.float32) * (NUM_HEADS * HEAD_DIM) ** -0.5).astype(jnp.bfloat16)
    w_gate_up = (jax.random.normal(shared_keys[4], (MODEL_DIM, 2 * FFN_DIM), jnp.float32) * MODEL_DIM ** -0.5).astype(jnp.bfloat16)
    w_down = (jax.random.normal(shared_keys[5], (FFN_DIM, MODEL_DIM), jnp.float32) * FFN_DIM ** -0.5).astype(jnp.bfloat16)
    pos_wave = jnp.cos(jnp.pi * jnp.arange(CACHE_LEN).astype(jnp.float32) / WINDOW)[None, :, None, None]
    key_dir = jax.random.normal(own_keys[3], (NUM_SEQS, 1, KV_HEADS, HEAD_DIM), jnp.float32)
    k_cache = (jax.random.normal(own_keys[2], cache_shape, jnp.float32) + key_dir * pos_wave).astype(jnp.bfloat16)
    v_trend = 2.0 * jax.random.normal(own_keys[5], (NUM_SEQS, 1, KV_HEADS, HEAD_DIM), jnp.float32)
    v_cache = (jax.random.normal(own_keys[4], cache_shape, jnp.float32) + v_trend * pos_wave).astype(jnp.bfloat16)
    return {'hidden': hidden, 'positions': positions, 'norm_attn': norm_attn, 'norm_mlp': norm_mlp, 'w_qkv': w_qkv, 'w_out': w_out, 'w_gate_up': w_gate_up, 'w_down': w_down, 'k_cache': k_cache, 'v_cache': v_cache}


def reference(hidden, positions, norm_attn, norm_mlp, w_qkv, w_out, w_gate_up, w_down, k_cache, v_cache):
    num_rows = hidden.shape[0]
    resid_in = hidden.astype(jnp.float32)
    normed = rms_norm(resid_in, norm_attn).astype(jnp.bfloat16)
    qkv_proj = jnp.dot(normed, w_qkv, preferred_element_type=jnp.float32).reshape(num_rows, KV_HEADS, GROUP_SIZE + 2, HEAD_DIM)
    cos_tab, sin_tab = rope_angles(positions)
    q_new = rotate_half(qkv_proj[:, :, :GROUP_SIZE], cos_tab[:, None, None], sin_tab[:, None, None]).astype(jnp.bfloat16)
    k_new = rotate_half(qkv_proj[:, :, GROUP_SIZE], cos_tab[:, None], sin_tab[:, None]).astype(jnp.bfloat16)
    v_new = qkv_proj[:, :, GROUP_SIZE + 1].astype(jnp.bfloat16)
    slot_ids = jnp.arange(CACHE_LEN)
    at_slot = (slot_ids[None, :] == positions[:, None])[:, :, None, None]
    k_upd = jnp.where(at_slot, k_new[:, None], k_cache)
    v_upd = jnp.where(at_slot, v_new[:, None], v_cache)
    attended = lax.map(seq_attention, (q_new, k_upd, v_upd, positions)).reshape(num_rows, NUM_HEADS * HEAD_DIM)
    out_parts = jnp.einsum('bsk,skd->bsd', attended.reshape(num_rows, TEN_PAR, -1).astype(jnp.float32), w_out.reshape(TEN_PAR, -1, MODEL_DIM).astype(jnp.float32))
    mid_resid = resid_in + jnp.sum(out_parts.astype(jnp.bfloat16).astype(jnp.float32), axis=1)
    normed_mlp = rms_norm(mid_resid, norm_mlp).astype(jnp.bfloat16)
    gate_up = jnp.dot(normed_mlp, w_gate_up, preferred_element_type=jnp.float32).reshape(num_rows, TEN_PAR, 2, FFN_LOCAL)
    act_vals = (jax.nn.silu(gate_up[:, :, 0]) * gate_up[:, :, 1]).astype(jnp.bfloat16)
    down_parts = jnp.einsum('bsf,sfd->bsd', act_vals.astype(jnp.float32), w_down.reshape(TEN_PAR, FFN_LOCAL, MODEL_DIM).astype(jnp.float32))
    result = mid_resid + jnp.sum(down_parts.astype(jnp.bfloat16).astype(jnp.float32), axis=1)
    return (result.astype(jnp.bfloat16), k_upd, v_upd)
```

```python
import functools

import jax
import jax.numpy as jnp
import numpy as np
from jax import lax
from jax.experimental import pallas as pl
from jax.experimental.pallas import tpu as pltpu
from jax.sharding import PartitionSpec as P

WINDOW = 2047
ROPE_BASE = 10000.0
NORM_EPS = 1e-5
MESH = pl.DeviceIdType.MESH
LANES = 128
QKV_CHUNKS = 4
VMEM_LIMIT = 60 * 1024 * 1024
F32, BF16 = jnp.float32, jnp.bfloat16


def dot(lhs, rhs):
    return jnp.dot(lhs, rhs, preferred_element_type=F32)


def dot_t(lhs, rhs):
    return lax.dot_general(lhs, rhs, (((1,), (1,)), ((), ())), preferred_element_type=F32)


def round_bf16(values):
    return values.astype(BF16).astype(F32)


def row_scale(values):
    return lax.rsqrt(jnp.mean(values * values, axis=-1, keepdims=True) + NORM_EPS)


def attend_kernel(dims, pos_ref, hid_ref, gain_ref, freq_ref, w_hbm, k_hbm, v_hbm, ko_hbm, vo_hbm, part_ref, resid_ref,
                  w_buf, k_buf, v_buf, norm_buf, proj_buf, q_buf, new_buf, w_sem, k_sem, v_sem, ko_sem, vo_sem):
    rows, block_len, kv_count, group, shares = dims
    heads = kv_count * group
    per_share = rows // shares
    w_rows = w_buf.shape[0] // QKV_CHUNKS

    def w_copy(c):
        part = pl.ds(c * w_rows, w_rows)
        return pltpu.make_async_copy(w_hbm.at[part], w_buf.at[part], w_sem.at[c])

    def cache_copy(src, dst, sem, g):
        part = pl.ds(g * per_share, per_share)
        return pltpu.make_async_copy(src.at[part], dst.at[part], sem.at[g])

    for c in range(QKV_CHUNKS):
        w_copy(c).start()
    for g in range(shares):
        cache_copy(k_hbm, k_buf, k_sem, g).start()
        cache_copy(v_hbm, v_buf, v_sem, g).start()

    resid = hid_ref[...].astype(F32)
    for s in range(shares):
        resid_ref[s] = resid[s * per_share:(s + 1) * per_share]
    norm_buf[...] = (resid * row_scale(resid) * gain_ref[...]).astype(BF16)

    row_id = lax.broadcasted_iota(jnp.int32, (8, LANES), 0)
    tiles = []
    for r in range(rows // 8):
        tile = jnp.zeros((8, LANES), jnp.int32)
        for i in range(8):
            tile = jnp.where(row_id == i, pos_ref[r * 8 + i], tile)
        tiles.append(tile)
    angles = jnp.concatenate(tiles, axis=0).astype(F32) * freq_ref[...]
    cos_tab = jnp.cos(angles)
    sin_tab = jnp.sin(angles)
    lane_id = lax.broadcasted_iota(jnp.int32, (rows, LANES), 1)
    sin_tab = jnp.where(lane_id < LANES // 2, -sin_tab, sin_tab)

    def rope(values):
        return values * cos_tab + pltpu.roll(values, LANES // 2, axis=1) * sin_tab

    for c in range(QKV_CHUNKS):
        part = slice(c * w_rows, (c + 1) * w_rows)
        w_copy(c).wait()
        term = dot(norm_buf[:, part], w_buf[part, :])
        proj_buf[...] = term if c == 0 else proj_buf[...] + term

    for kv in range(kv_count):
        base = kv * (group + 2) * LANES
        for g in range(group):
            q_new = round_bf16(rope(proj_buf[:, base + g * LANES:base + (g + 1) * LANES]))
            q_buf[pl.ds(kv * group + g, rows, stride=heads), :] = q_new
        k_col = base + group * LANES
        new_buf[pl.ds(kv, rows, stride=8), :] = round_bf16(rope(proj_buf[:, k_col:k_col + LANES]))
        new_buf[pl.ds(kv_count + kv, rows, stride=8), :] = round_bf16(proj_buf[:, k_col + LANES:k_col + 2 * LANES])

    start = lax.axis_index('sp') * block_len
    score_scale = LANES ** -0.5
    tile_rows = 8 * kv_count
    tile_id = lax.broadcasted_iota(jnp.int32, (tile_rows, LANES), 0)
    col_id = lax.broadcasted_iota(jnp.int32, (heads, block_len * kv_count), 1)
    head_id = lax.broadcasted_iota(jnp.int32, (heads, block_len * kv_count), 0)
    own_kv = lax.rem(col_id, kv_count) == head_id // group
    slot_id = jnp.where(own_kv, start + col_id // kv_count, -1)
    stat_lane = lax.broadcasted_iota(jnp.int32, (heads, LANES), 1)

    def write_row(buf, b, slot, first):
        base = pl.multiple_of((slot // 8) * tile_rows, tile_rows)
        tile = buf[b, pl.ds(base, tile_rows), :].astype(F32)
        lines = new_buf[pl.ds(pl.multiple_of(b * 8, 8), 8), :]
        new = jnp.zeros((tile_rows, LANES), F32)
        for kv in range(kv_count):
            line = lines[first + kv:first + kv + 1, :]
            new = jnp.where(lax.rem(tile_id, kv_count) == kv, line, new)
        hit = tile_id // kv_count == lax.rem(slot, 8)
        buf[b, pl.ds(base, tile_rows), :] = jnp.where(hit, new, tile).astype(BF16)

    def share_step(g, carry):
        cache_copy(k_hbm, k_buf, k_sem, g).wait()
        cache_copy(v_hbm, v_buf, v_sem, g).wait()
        for i in range(per_share):
            b = g * per_share + i
            slot = pos_ref[b] - start

            @pl.when(jnp.logical_and(slot >= 0, slot < block_len))
            def _():
                write_row(k_buf, b, slot, 0)
                write_row(v_buf, b, slot, kv_count)

        cache_copy(k_buf, ko_hbm, ko_sem, g).start()
        cache_copy(v_buf, vo_hbm, vo_sem, g).start()
        stats = jnp.zeros((heads, LANES), F32)
        for i in range(per_share):
            b = g * per_share + i
            pos = pos_ref[b]
            q_rows = q_buf[pl.ds(pl.multiple_of(b * heads, heads), heads), :].astype(BF16)
            scores = dot_t(q_rows, k_buf[b]) * score_scale
            seen = (slot_id <= pos) & (slot_id >= jnp.maximum(pos - WINDOW, 0))
            scores = jnp.where(seen, scores, -jnp.inf)
            top = jnp.max(scores, axis=-1, keepdims=True)
            base = jnp.where(top == -jnp.inf, 0.0, top)
            weights = jnp.exp(scores - base)
            total = jnp.sum(weights, axis=-1, keepdims=True)
            part_ref[g, i] = dot(weights.astype(BF16), v_buf[b])
            stats = jnp.where(stat_lane == i, top, stats)
            stats = jnp.where(stat_lane == per_share + i, total, stats)
        part_ref[g, per_share] = stats
        return carry

    lax.fori_loop(0, shares, share_step, 0)
    for g in range(shares):
        cache_copy(k_buf, ko_hbm, ko_sem, g).wait()
        cache_copy(v_buf, vo_hbm, vo_sem, g).wait()


def tail_kernel(n_tp, n_sp, part_ref, resid_hbm, gain_ref, wo_hbm, wgu_hbm, wd_hbm, out_ref,
                wo_buf, wg_buf, wu_buf, wd_buf, resid_buf, part_in, att_buf, y1_buf, x1_in, x1_buf, r2_buf,
                a_out, a_in, y2_buf, x2_in, w_sem, b_send, b_recv, y1_send, y1_recv, g1_send, g1_recv,
                a_send, a_recv, y2_send, y2_recv, g2_send, g2_recv):
    t = lax.axis_index('tp')
    s = lax.axis_index('sp')
    chip, core = s // 2, lax.rem(s, 2)
    n_chip = n_sp // 2
    mate = chip * 2 + 1 - core
    units = wd_hbm.shape[0]
    chip_tiles = units // LANES // n_chip
    core_tiles = (chip_tiles + 1) // 2
    width = core_tiles * LANES
    model = wo_hbm.shape[1]
    half = model // 2
    col = pl.multiple_of((chip * chip_tiles + core * (chip_tiles - core_tiles)) * LANES, LANES)
    loads = [
        pltpu.make_async_copy(resid_hbm.at[s], resid_buf, w_sem.at[0]),
        pltpu.make_async_copy(wo_hbm, wo_buf, w_sem.at[1]),
        pltpu.make_async_copy(wgu_hbm.at[:, pl.ds(col, width)], wg_buf, w_sem.at[2]),
        pltpu.make_async_copy(wgu_hbm.at[:, pl.ds(pl.multiple_of(units + col, LANES), width)], wu_buf, w_sem.at[3]),
        pltpu.make_async_copy(wd_hbm.at[:, pl.ds(pl.multiple_of(core * half, half), half)], wd_buf, w_sem.at[4]),
    ]
    for load in loads:
        load.start()

    def sp_at(k):
        return lax.rem(s + k, n_sp)

    def sp_from(k):
        return lax.rem(s + n_sp - k, n_sp)

    def tp_at(k):
        return lax.rem(t + k, n_tp)

    def tp_from(k):
        return lax.rem(t + n_tp - k, n_tp)

    barrier = pltpu.get_barrier_semaphore()
    for k in range(1, n_sp):
        pl.semaphore_signal(barrier, inc=1, device_id={'sp': sp_at(k)}, device_id_type=MESH)
    for k in range(1, n_tp):
        pl.semaphore_signal(barrier, inc=1, device_id={'tp': tp_at(k)}, device_id_type=MESH)
    pl.semaphore_wait(barrier, n_sp + n_tp - 2)

    def remote(src, dst, send, recv, device):
        return pltpu.make_async_remote_copy(src_ref=src, dst_ref=dst, send_sem=send, recv_sem=recv,
                                            device_id=device, device_id_type=MESH)

    def exchange_sp(src_of, buf, send, recv):
        copies = [remote(src_of(sp_at(k)), buf.at[s], send.at[k - 1], recv.at[k - 1], {'sp': sp_at(k)}) for k in range(1, n_sp)]
        for copy in copies:
            copy.start()

        def finish():
            for k in range(1, n_sp):
                remote(buf.at[s], buf.at[sp_from(k)], send.at[k - 1], recv.at[k - 1], {'sp': sp_at(k)}).wait_recv()
            for copy in copies:
                copy.wait_send()
        return finish

    def exchange_tp(buf, send, recv):
        copies = [remote(buf.at[t], buf.at[t], send.at[k - 1], recv.at[k - 1], {'tp': tp_at(k)}) for k in range(1, n_tp)]
        for copy in copies:
            copy.start()
        for k in range(1, n_tp):
            remote(buf.at[t], buf.at[tp_from(k)], send.at[k - 1], recv.at[k - 1], {'tp': tp_at(k)}).wait_recv()
        for copy in copies:
            copy.wait_send()

    def gather_sp(buf, send, recv):
        def far(k):
            return lax.rem(chip + k, n_chip) * 2 + core

        def far_from(k, c):
            return lax.rem(chip + n_chip - k, n_chip) * 2 + c
        copies = [remote(buf.at[s], buf.at[s], send.at[k], recv.at[k], {'sp': far(k)}) for k in range(1, n_chip)]
        copies.append(remote(buf.at[s], buf.at[s], send.at[0], recv.at[0], {'sp': mate}))
        for copy in copies:
            copy.start()
        for k in sorted(range(1, n_chip), key=lambda k: min(k, n_chip - k)):
            slot = far_from(k, core)
            remote(buf.at[s], buf.at[slot], send.at[k], recv.at[k], {'sp': far(k)}).wait_recv()
            relay = remote(buf.at[slot], buf.at[slot], send.at[n_chip + k - 1], recv.at[n_chip + k - 1], {'sp': mate})
            relay.start()
            copies.append(relay)
        remote(buf.at[s], buf.at[mate], send.at[0], recv.at[0], {'sp': mate}).wait_recv()
        for k in range(1, n_chip):
            slot = far_from(k, 1 - core)
            remote(buf.at[s], buf.at[slot], send.at[n_chip + k - 1], recv.at[n_chip + k - 1], {'sp': mate}).wait_recv()
        for copy in copies:
            copy.wait_send()

    per_share = part_ref.shape[1] - 1
    heads = part_ref.shape[2]
    finish = exchange_sp(lambda peer: part_ref.at[peer], part_in, b_send, b_recv)
    part_in[s] = part_ref[s]
    finish()
    stats = [part_in[j, per_share] for j in range(n_sp)]
    top = functools.reduce(jnp.maximum, stats)
    scales = [jnp.exp(st - top) for st in stats]
    total = sum(sc * pltpu.roll(st, LANES - per_share, axis=1) for sc, st in zip(scales, stats))
    for i in range(per_share):
        acc = sum(part_in[j, i] * scales[j][:, i:i + 1] for j in range(n_sp))
        att_buf[i * heads:(i + 1) * heads, :] = round_bf16(acc / total[:, i:i + 1])
    attended = jnp.concatenate([att_buf[pl.ds(h, per_share, stride=heads), :] for h in range(heads)], axis=1).astype(BF16)

    loads[0].wait()
    loads[1].wait()
    y1_buf[t] = round_bf16(dot(attended, wo_buf[...]))
    exchange_tp(y1_buf, y1_send, y1_recv)
    out_sum = functools.reduce(jnp.add, [y1_buf[j] for j in range(n_tp)])
    x1_in[s] = resid_buf[...] + out_sum
    gather_sp(x1_in, g1_send, g1_recv)

    rows = n_sp * per_share
    for j in range(n_sp):
        x1_buf[j * per_share:(j + 1) * per_share, :] = x1_in[j]
    chunk = 4 * LANES
    square = jnp.zeros((rows, LANES), F32)
    for c in range(model // LANES):
        piece = x1_buf[:, c * LANES:(c + 1) * LANES]
        square = square + piece * piece
    scale = lax.rsqrt(jnp.sum(square, axis=-1, keepdims=True) / model + NORM_EPS)
    for c in range(model // chunk):
        part = slice(c * chunk, (c + 1) * chunk)
        r2_buf[:, part] = (x1_buf[:, part] * scale * gain_ref[:, part]).astype(BF16)

    loads[2].wait()
    gate = dot(r2_buf[...], wg_buf[...])
    loads[3].wait()
    up = dot(r2_buf[...], wu_buf[...])
    act = round_bf16(gate * jax.nn.sigmoid(gate) * up)
    chip_rows = 2 * per_share
    for j in range(n_chip):
        a_out[j] = act[j * chip_rows:(j + 1) * chip_rows]
    finish = exchange_sp(lambda peer: a_out.at[peer // 2], a_in, a_send, a_recv)
    a_in[s] = a_out[chip]
    finish()
    pieces = []
    for j in range(n_chip):
        pieces.append(a_in[2 * j])
        pieces.append(a_in[2 * j + 1][:, (2 * core_tiles - chip_tiles) * LANES:])
    act_rows = jnp.concatenate(pieces, axis=1).astype(BF16)

    loads[4].wait()
    y2_buf[t] = round_bf16(dot(act_rows, wd_buf[...]))
    exchange_tp(y2_buf, y2_send, y2_recv)
    down_sum = functools.reduce(jnp.add, [y2_buf[j] for j in range(n_tp)])
    own = x1_buf[pl.ds(pl.multiple_of(chip * chip_rows, chip_rows), chip_rows), pl.ds(pl.multiple_of(core * half, half), half)]
    x2_in[s] = own + down_sum
    gather_sp(x2_in, g2_send, g2_recv)
    for j in range(0, n_chip, 2):
        for c in range(2):
            pair = jnp.concatenate([x2_in[2 * j + c], x2_in[2 * j + 2 + c]], axis=0)
            out_ref[j * chip_rows:(j + 2) * chip_rows, c * half:(c + 1) * half] = pair.astype(BF16)


def vmem():
    return pl.BlockSpec(memory_space=pltpu.VMEM)


def hbm():
    return pl.BlockSpec(memory_space=pl.ANY)


def solution(mesh):
    n_tp, n_sp = mesh.shape['tp'], mesh.shape['sp']
    cache_spec = P('dp', 'sp', 'tp', None)

    def local_step(hidden, positions, norm_attn, norm_mlp, w_qkv, w_out, w_gate_up, w_down, k_cache, v_cache):
        rows, block_len, kv_count, head_dim = k_cache.shape
        model = hidden.shape[1]
        group = w_qkv.shape[1] // (kv_count * head_dim) - 2
        heads = kv_count * group
        shares = n_sp
        per_share = rows // shares
        flat = (rows, block_len * kv_count, head_dim)
        inv_freq = ROPE_BASE ** (-np.arange(0, head_dim, 2) / head_dim)
        freq = jnp.asarray(np.concatenate([inv_freq, inv_freq])[None, :], F32)
        dma = pltpu.SemaphoreType.DMA

        k_upd, v_upd, parts, resid = pl.pallas_call(
            functools.partial(attend_kernel, (rows, block_len, kv_count, group, shares)),
            out_shape=(
                jax.ShapeDtypeStruct(flat, BF16),
                jax.ShapeDtypeStruct(flat, BF16),
                jax.ShapeDtypeStruct((shares, per_share + 1, heads, head_dim), F32),
                jax.ShapeDtypeStruct((shares, per_share, model), F32),
            ),
            in_specs=[pl.BlockSpec(memory_space=pltpu.SMEM), vmem(), vmem(), vmem(), hbm(), hbm(), hbm()],
            out_specs=(hbm(), hbm(), vmem(), vmem()),
            scratch_shapes=[
                pltpu.VMEM(w_qkv.shape, BF16),
                pltpu.VMEM(flat, BF16),
                pltpu.VMEM(flat, BF16),
                pltpu.VMEM((rows, model), BF16),
                pltpu.VMEM((rows, w_qkv.shape[1]), F32),
                pltpu.VMEM((rows * heads, head_dim), F32),
                pltpu.VMEM((rows * 8, head_dim), F32),
                dma((QKV_CHUNKS,)), dma((shares,)), dma((shares,)), dma((shares,)), dma((shares,)),
            ],
            compiler_params=pltpu.CompilerParams(vmem_limit_bytes=VMEM_LIMIT),
            name='attend',
        )(positions, hidden, norm_attn[None, :], freq, w_qkv, k_cache.reshape(flat), v_cache.reshape(flat))

        units = w_down.shape[0]
        n_chip = n_sp // 2
        chip_tiles = units // LANES // n_chip
        width = (chip_tiles + 1) // 2 * LANES
        chip_rows = 2 * per_share
        half = model // 2
        result = pl.pallas_call(
            functools.partial(tail_kernel, n_tp, n_sp),
            out_shape=jax.ShapeDtypeStruct((rows, model), BF16),
            in_specs=[vmem(), hbm(), vmem(), hbm(), hbm(), hbm()],
            out_specs=vmem(),
            scratch_shapes=[
                pltpu.VMEM(w_out.shape, BF16),
                pltpu.VMEM((model, width), BF16),
                pltpu.VMEM((model, width), BF16),
                pltpu.VMEM((units, half), BF16),
                pltpu.VMEM((per_share, model), F32),
                pltpu.VMEM((n_sp, per_share + 1, heads, head_dim), F32),
                pltpu.VMEM((per_share * heads, head_dim), F32),
                pltpu.VMEM((n_tp, per_share, model), F32),
                pltpu.VMEM((n_sp, per_share, model), F32),
                pltpu.VMEM((rows, model), F32),
                pltpu.VMEM((rows, model), BF16),
                pltpu.VMEM((n_chip, chip_rows, width), F32),
                pltpu.VMEM((n_sp, chip_rows, width), F32),
                pltpu.VMEM((n_tp, chip_rows, half), F32),
                pltpu.VMEM((n_sp, chip_rows, half), F32),
                dma((5,)),
                dma((n_sp - 1,)), dma((n_sp - 1,)),
                dma((n_tp - 1,)), dma((n_tp - 1,)),
                dma((n_sp - 1,)), dma((n_sp - 1,)),
                dma((n_sp - 1,)), dma((n_sp - 1,)),
                dma((n_tp - 1,)), dma((n_tp - 1,)),
                dma((n_sp - 1,)), dma((n_sp - 1,)),
            ],
            compiler_params=pltpu.CompilerParams(vmem_limit_bytes=VMEM_LIMIT, collective_id=0, has_side_effects=True),
            name='tail',
        )(parts, resid, norm_mlp[None, :], w_out, w_gate_up, w_down)
        return result, k_upd.reshape(k_cache.shape), v_upd.reshape(v_cache.shape)

    return jax.shard_map(local_step, mesh=mesh, in_specs=(P('dp', None), P('dp'), P(None), P(None), P(None, 'tp'), P('tp', None), P(None, 'tp'), P('tp', None), cache_spec, cache_spec), out_specs=(P('dp', None), cache_spec, cache_spec), check_vma=False)
```

```python
import functools

import jax
import jax.numpy as jnp
import numpy as np
from jax import lax
from jax.experimental import pallas as pl
from jax.experimental.pallas import tpu as pltpu
from jax.sharding import PartitionSpec as P

WINDOW = 2047
ROPE_BASE = 10000.0
NORM_EPS = 1e-5
MESH = pl.DeviceIdType.MESH
LANES = 128
QKV_CHUNKS = 4
CHUNKS = 4
VMEM_LIMIT = 60 * 1024 * 1024
F32, BF16 = jnp.float32, jnp.bfloat16


def dot(lhs, rhs):
    return jnp.dot(lhs, rhs, preferred_element_type=F32)


def dot_t(lhs, rhs):
    return lax.dot_general(lhs, rhs, (((1,), (1,)), ((), ())), preferred_element_type=F32)


def round_bf16(values):
    return values.astype(BF16).astype(F32)


def row_scale(values):
    return lax.rsqrt(jnp.mean(values * values, axis=-1, keepdims=True) + NORM_EPS)


def attend_kernel(dims, pos_hbm, hid_hbm, gain_hbm, freq_hbm, w_hbm, k_hbm, v_hbm, ko_hbm, vo_hbm, part_hbm, resid_hbm,
                  pos_ref, hid_ref, gain_ref, freq_ref, w_buf, k_buf, v_buf, norm_buf, proj_buf, q_buf, new_buf, s_buf,
                  part_ref, resid_ref, in_sem, w_sem, k_sem, v_sem, ko_sem, vo_sem, out_sem):
    rows, block_len, kv_count, group, shares = dims
    heads = kv_count * group
    per_share = rows // shares
    w_rows = w_buf.shape[0] // QKV_CHUNKS

    def w_copy(c):
        part = pl.ds(c * w_rows, w_rows)
        return pltpu.make_async_copy(w_hbm.at[part], w_buf.at[part], w_sem.at[c])

    def cache_copy(src, dst, sem, g):
        part = pl.ds(g * per_share, per_share)
        return pltpu.make_async_copy(src.at[part], dst.at[part], sem.at[g])

    small = [pltpu.make_async_copy(src, dst, in_sem.at[n]) for n, (src, dst) in enumerate(
        [(hid_hbm, hid_ref), (gain_hbm, gain_ref), (freq_hbm, freq_ref), (pos_hbm, pos_ref)])]
    for copy in small:
        copy.start()
    for c in range(QKV_CHUNKS):
        w_copy(c).start()
    for g in range(shares):
        cache_copy(k_hbm, k_buf, k_sem, g).start(priority=1)
    for copy in small:
        copy.wait()

    resid = hid_ref[...].astype(F32)
    for s in range(shares):
        resid_ref[s] = resid[s * per_share:(s + 1) * per_share]
    resid_copy = pltpu.make_async_copy(resid_ref, resid_hbm, out_sem.at[0])
    resid_copy.start()
    norm_buf[...] = (resid * row_scale(resid) * gain_ref[...]).astype(BF16)

    row_id = lax.broadcasted_iota(jnp.int32, (8, LANES), 0)
    tiles = []
    for r in range(rows // 8):
        tile = jnp.zeros((8, LANES), jnp.int32)
        for i in range(8):
            tile = jnp.where(row_id == i, pos_ref[r * 8 + i], tile)
        tiles.append(tile)
    angles = jnp.concatenate(tiles, axis=0).astype(F32) * freq_ref[...]
    cos_tab = jnp.cos(angles)
    sin_tab = jnp.sin(angles)
    lane_id = lax.broadcasted_iota(jnp.int32, (rows, LANES), 1)
    sin_tab = jnp.where(lane_id < LANES // 2, -sin_tab, sin_tab)

    def rope(values):
        return values * cos_tab + pltpu.roll(values, LANES // 2, axis=1) * sin_tab

    for c in range(QKV_CHUNKS):
        part = slice(c * w_rows, (c + 1) * w_rows)
        w_copy(c).wait()
        if c == QKV_CHUNKS - 1:
            for g in range(shares):
                cache_copy(v_hbm, v_buf, v_sem, g).start()
        term = dot(norm_buf[:, part], w_buf[part, :])
        proj_buf[...] = term if c == 0 else proj_buf[...] + term

    for kv in range(kv_count):
        base = kv * (group + 2) * LANES
        for g in range(group):
            q_new = round_bf16(rope(proj_buf[:, base + g * LANES:base + (g + 1) * LANES]))
            q_buf[pl.ds(kv * group + g, rows, stride=heads), :] = q_new
        k_col = base + group * LANES
        new_buf[pl.ds(kv, rows, stride=8), :] = round_bf16(rope(proj_buf[:, k_col:k_col + LANES]))
        new_buf[pl.ds(kv_count + kv, rows, stride=8), :] = round_bf16(proj_buf[:, k_col + LANES:k_col + 2 * LANES])

    start = lax.axis_index('sp') * block_len
    score_scale = LANES ** -0.5
    tile_rows = 8 * kv_count
    tile_id = lax.broadcasted_iota(jnp.int32, (tile_rows, LANES), 0)
    col_id = lax.broadcasted_iota(jnp.int32, (heads, block_len * kv_count), 1)
    head_id = lax.broadcasted_iota(jnp.int32, (heads, block_len * kv_count), 0)
    own_kv = lax.rem(col_id, kv_count) == head_id // group
    slot_id = jnp.where(own_kv, start + col_id // kv_count, -1)
    stat_lane = lax.broadcasted_iota(jnp.int32, (heads, LANES), 1)

    def write_row(buf, b, first):
        slot = pos_ref[b] - start

        @pl.when(jnp.logical_and(slot >= 0, slot < block_len))
        def _():
            base = pl.multiple_of((slot // 8) * tile_rows, tile_rows)
            tile = buf[b, pl.ds(base, tile_rows), :].astype(F32)
            lines = new_buf[pl.ds(pl.multiple_of(b * 8, 8), 8), :]
            new = jnp.zeros((tile_rows, LANES), F32)
            for kv in range(kv_count):
                line = lines[first + kv:first + kv + 1, :]
                new = jnp.where(lax.rem(tile_id, kv_count) == kv, line, new)
            hit = tile_id // kv_count == lax.rem(slot, 8)
            buf[b, pl.ds(base, tile_rows), :] = jnp.where(hit, new, tile).astype(BF16)

    def key_step(g, carry):
        cache_copy(k_hbm, k_buf, k_sem, g).wait()
        for i in range(per_share):
            write_row(k_buf, g * per_share + i, 0)
        cache_copy(k_buf, ko_hbm, ko_sem, g).start(priority=1)
        for i in range(per_share):
            b = g * per_share + i
            q_rows = q_buf[pl.ds(pl.multiple_of(b * heads, heads), heads), :].astype(BF16)
            s_buf[b] = dot_t(q_rows, k_buf[b])
        return carry

    def weight_step(g, carry):
        stats = jnp.zeros((heads, LANES), F32)
        for i in range(per_share):
            b = g * per_share + i
            pos = pos_ref[b]
            seen = (slot_id <= pos) & (slot_id >= jnp.maximum(pos - WINDOW, 0))
            scores = jnp.where(seen, s_buf[b] * score_scale, -jnp.inf)
            top = jnp.max(scores, axis=-1, keepdims=True)
            base = jnp.where(top == -jnp.inf, 0.0, top)
            weights = jnp.exp(scores - base)
            total = jnp.sum(weights, axis=-1, keepdims=True)
            s_buf[b] = weights
            stats = jnp.where(stat_lane == i, top, stats)
            stats = jnp.where(stat_lane == per_share + i, total, stats)
        part_ref[g, per_share] = stats
        return carry

    def value_step(g, carry):
        cache_copy(v_hbm, v_buf, v_sem, g).wait()
        for i in range(per_share):
            write_row(v_buf, g * per_share + i, kv_count)
        cache_copy(v_buf, vo_hbm, vo_sem, g).start(priority=1)
        for i in range(per_share):
            b = g * per_share + i
            part_ref[g, i] = dot(s_buf[b].astype(BF16), v_buf[b])
        return carry

    lax.fori_loop(0, shares, key_step, 0)
    lax.fori_loop(0, shares, weight_step, 0)
    lax.fori_loop(0, shares, value_step, 0)
    part_copy = pltpu.make_async_copy(part_ref, part_hbm, out_sem.at[1])
    part_copy.start()
    for g in range(shares):
        cache_copy(k_buf, ko_hbm, ko_sem, g).wait()
        cache_copy(v_buf, vo_hbm, vo_sem, g).wait()
    resid_copy.wait()
    part_copy.wait()


def tail_kernel(n_tp, n_sp, part_ref, resid_hbm, gain_ref, wo_hbm, wgu_hbm, wd_hbm, out_ref,
                wo_buf, wgu_buf, wd_buf, resid_buf, part_in, att_buf, y1_buf, x1_in, x1_buf, r2_buf,
                a_out, a_in, y2_buf, x2_in, w_sem, b_send, b_recv, y1_send, y1_recv, g1_send, g1_recv,
                a_send, a_recv, y2_send, y2_recv, g2_send, g2_recv):
    t = lax.axis_index('tp')
    s = lax.axis_index('sp')
    n_chip = n_sp // 2
    chip, core = s // 2, lax.rem(s, 2)
    mate = chip * 2 + 1 - core
    units, model = wd_hbm.shape
    chip_units = units // n_chip
    splits = unit_splits(chip_units)
    half = model // 2
    per_share = part_ref.shape[1] - 1
    heads = part_ref.shape[2]
    half_rows = n_chip * per_share
    group_rows = 2 * per_share

    def group_of(dev):
        return lax.rem(dev, 2) * n_chip + dev // 2

    resid_load = pltpu.make_async_copy(resid_hbm.at[group_of(s)], resid_buf, w_sem.at[0])
    wo_load = pltpu.make_async_copy(wo_hbm, wo_buf, w_sem.at[1])
    gu_loads = []
    at = 0
    for first, width in splits:
        for side in range(2):
            col = pl.multiple_of(side * units + chip * chip_units + first, LANES)
            gu_loads.append(pltpu.make_async_copy(wgu_hbm.at[:, pl.ds(col, width)], wgu_buf.at[:, pl.ds(at, width)], w_sem.at[2 + len(gu_loads)]))
            at += width
    wd_col = pl.multiple_of(lax.rem(chip, 2) * half, half)
    wd_load = pltpu.make_async_copy(wd_hbm.at[:, pl.ds(wd_col, half)], wd_buf, w_sem.at[6])
    resid_load.start()
    wo_load.start()

    def wrap(value, count):
        return lax.rem(value + count, count)

    barrier = pltpu.get_barrier_semaphore()
    for k in range(1, n_sp):
        pl.semaphore_signal(barrier, inc=1, device_id={'sp': wrap(s + k, n_sp)}, device_id_type=MESH)
    for k in range(1, n_tp):
        pl.semaphore_signal(barrier, inc=1, device_id={'tp': wrap(t + k, n_tp)}, device_id_type=MESH)
    pl.semaphore_wait(barrier, n_sp + n_tp - 2)

    sent = []

    def push(src, dst, send, recv, device):
        copy = pltpu.make_async_remote_copy(src_ref=src, dst_ref=dst, send_sem=send, recv_sem=recv, device_id=device, device_id_type=MESH)
        copy.start()
        sent.append(copy)

    def arrive(dst, recv):
        pltpu.make_async_remote_copy(src_ref=dst, dst_ref=dst, send_sem=b_send.at[0], recv_sem=recv, device_id={'sp': mate}, device_id_type=MESH).wait_recv()

    near_first = sorted(range(1, n_chip), key=lambda k: min(k, n_chip - k))

    def peer(k):
        return {'sp': wrap(chip + k, n_chip) * 2 + core}

    for k in range(1, n_sp):
        dev = wrap(s + k, n_sp)
        push(part_ref.at[group_of(dev)], part_in.at[s], b_send.at[k - 1], b_recv.at[k - 1], {'sp': dev})
    part_in[s] = part_ref[group_of(s)]
    resid_load.wait()
    wo_load.wait()
    for load in gu_loads:
        load.start()
    for k in range(1, n_sp):
        arrive(part_in.at[wrap(s - k, n_sp)], b_recv.at[k - 1])
    stats = [part_in[j, per_share] for j in range(n_sp)]
    top = functools.reduce(jnp.maximum, stats)
    scales = [jnp.exp(st - top) for st in stats]
    total = sum(sc * pltpu.roll(st, LANES - per_share, axis=1) for sc, st in zip(scales, stats))
    for i in range(per_share):
        acc = sum(part_in[j, i] * scales[j][:, i:i + 1] for j in range(n_sp))
        att_buf[i * heads:(i + 1) * heads, :] = round_bf16(acc / total[:, i:i + 1])
    attended = jnp.concatenate([att_buf[pl.ds(h, per_share, stride=heads), :] for h in range(heads)], axis=1).astype(BF16)

    width = model // CHUNKS
    for n in range(CHUNKS):
        y1_buf[n, t] = round_bf16(dot(attended, wo_buf[:, n * width:(n + 1) * width]))
        for k in range(1, n_tp):
            push(y1_buf.at[n, t], y1_buf.at[n, t], y1_send.at[n, k - 1], y1_recv.at[n, k - 1], {'tp': wrap(t + k, n_tp)})
    wd_load.start()
    for n in range(CHUNKS):
        for k in range(1, n_tp):
            arrive(y1_buf.at[n, wrap(t - k, n_tp)], y1_recv.at[n, k - 1])
        out_sum = functools.reduce(jnp.add, [y1_buf[n, j] for j in range(n_tp)])
        x1_in[n, chip] = resid_buf[:, n * width:(n + 1) * width] + out_sum
        for k in near_first:
            push(x1_in.at[n, chip], x1_in.at[n, chip], g1_send.at[n, k - 1], g1_recv.at[n, k - 1], peer(k))
    square = jnp.zeros((half_rows, LANES), F32)
    for n in range(CHUNKS):
        for k in near_first:
            arrive(x1_in.at[n, wrap(chip - k, n_chip)], g1_recv.at[n, k - 1])
        for j in range(n_chip):
            x1_buf[j * per_share:(j + 1) * per_share, n * width:(n + 1) * width] = x1_in[n, j]
        for c in range(width // LANES):
            piece = x1_buf[:, n * width + c * LANES:n * width + (c + 1) * LANES]
            square = square + piece * piece
    scale = lax.rsqrt(jnp.sum(square, axis=-1, keepdims=True) / model + NORM_EPS)
    for c in range(0, model, 4 * LANES):
        part = slice(c, c + 4 * LANES)
        r2_buf[:, part] = (x1_buf[:, part] * scale * gain_ref[:, part]).astype(BF16)

    at = 0
    for n, (first, width) in enumerate(splits):
        gu_loads[2 * n].wait()
        gu_loads[2 * n + 1].wait()
        both = dot(r2_buf[...], wgu_buf[:, at:at + 2 * width])
        at += 2 * width
        gate = both[:, :width]
        act = round_bf16(gate * jax.nn.sigmoid(gate) * both[:, width:])
        for j in range(half_rows // group_rows):
            a_out[j, :, first:first + width] = act[j * group_rows:(j + 1) * group_rows]
        for k in near_first:
            dst = wrap(chip + k, n_chip)
            push(a_out.at[dst // 2, :, pl.ds(first, width)], a_in.at[chip, :, pl.ds(first, width)],
                 a_send.at[n, k - 1], a_recv.at[n, k - 1], peer(k))
    a_in[chip] = a_out[chip // 2]
    wd_load.wait()
    for n, (first, width) in enumerate(splits):
        for k in near_first:
            arrive(a_in.at[wrap(chip - k, n_chip), :, pl.ds(first, width)], a_recv.at[n, k - 1])
    act_rows = jnp.concatenate([a_in[j] for j in range(n_chip)], axis=1).astype(BF16)

    width = half // CHUNKS
    for n in range(CHUNKS):
        y2_buf[n, t] = round_bf16(dot(act_rows, wd_buf[:, n * width:(n + 1) * width]))
        for k in range(1, n_tp):
            push(y2_buf.at[n, t], y2_buf.at[n, t], y2_send.at[n, k - 1], y2_recv.at[n, k - 1], {'tp': wrap(t + k, n_tp)})
    own_rows = pl.ds(pl.multiple_of(chip // 2 * group_rows, group_rows), group_rows)
    for n in range(CHUNKS):
        for k in range(1, n_tp):
            arrive(y2_buf.at[n, wrap(t - k, n_tp)], y2_recv.at[n, k - 1])
        down_sum = functools.reduce(jnp.add, [y2_buf[n, j] for j in range(n_tp)])
        x2_in[n, s] = x1_buf[own_rows, pl.ds(pl.multiple_of(wd_col + n * width, width), width)] + down_sum
        for k in near_first:
            push(x2_in.at[n, s], x2_in.at[n, s], g2_send.at[n, k], g2_recv.at[n, k], peer(k))
        push(x2_in.at[n, s], x2_in.at[n, s], g2_send.at[n, 0], g2_recv.at[n, 0], {'sp': mate})
    for n in range(CHUNKS):
        for k in near_first:
            far = x2_in.at[n, wrap(chip - k, n_chip) * 2 + core]
            arrive(far, g2_recv.at[n, k])
            push(far, far, g2_send.at[n, n_chip + k - 1], g2_recv.at[n, n_chip + k - 1], {'sp': mate})
    for n in range(CHUNKS):
        arrive(x2_in.at[n, mate], g2_recv.at[n, 0])
        for k in near_first:
            arrive(x2_in.at[n, wrap(chip - k, n_chip) * 2 + 1 - core], g2_recv.at[n, n_chip + k - 1])
        for c in range(2):
            for side in range(2):
                lines = jnp.concatenate([x2_in[n, 2 * j + c] for j in range(side, n_chip, 2)], axis=0)
                col = side * half + n * width
                out_ref[c * half_rows:(c + 1) * half_rows, col:col + width] = lines.astype(BF16)
    for copy in sent:
        copy.wait_send()


def unit_splits(count):
    first = (count // LANES + 1) // 2 * LANES
    return [(0, first), (first, count - first)]


def vmem():
    return pl.BlockSpec(memory_space=pltpu.VMEM)


def hbm():
    return pl.BlockSpec(memory_space=pl.ANY)


def solution(mesh):
    n_tp, n_sp = mesh.shape['tp'], mesh.shape['sp']
    cache_spec = P('dp', 'sp', 'tp', None)

    def local_step(hidden, positions, norm_attn, norm_mlp, w_qkv, w_out, w_gate_up, w_down, k_cache, v_cache):
        rows, block_len, kv_count, head_dim = k_cache.shape
        model = hidden.shape[1]
        group = w_qkv.shape[1] // (kv_count * head_dim) - 2
        heads = kv_count * group
        shares = n_sp
        per_share = rows // shares
        flat = (rows, block_len * kv_count, head_dim)
        inv_freq = ROPE_BASE ** (-np.arange(0, head_dim, 2) / head_dim)
        freq = jnp.asarray(np.concatenate([inv_freq, inv_freq])[None, :], F32)
        dma = pltpu.SemaphoreType.DMA

        k_upd, v_upd, parts, resid = pl.pallas_call(
            functools.partial(attend_kernel, (rows, block_len, kv_count, group, shares)),
            out_shape=(
                jax.ShapeDtypeStruct(flat, BF16),
                jax.ShapeDtypeStruct(flat, BF16),
                jax.ShapeDtypeStruct((shares, per_share + 1, heads, head_dim), F32),
                jax.ShapeDtypeStruct((shares, per_share, model), F32),
            ),
            in_specs=[hbm()] * 7,
            out_specs=(hbm(), hbm(), hbm(), hbm()),
            scratch_shapes=[
                pltpu.SMEM(positions.shape, jnp.int32),
                pltpu.VMEM(hidden.shape, BF16),
                pltpu.VMEM((1, model), F32),
                pltpu.VMEM(freq.shape, F32),
                pltpu.VMEM(w_qkv.shape, BF16),
                pltpu.VMEM(flat, BF16),
                pltpu.VMEM(flat, BF16),
                pltpu.VMEM((rows, model), BF16),
                pltpu.VMEM((rows, w_qkv.shape[1]), F32),
                pltpu.VMEM((rows * heads, head_dim), F32),
                pltpu.VMEM((rows * 8, head_dim), F32),
                pltpu.VMEM((rows, heads, block_len * kv_count), F32),
                pltpu.VMEM((shares, per_share + 1, heads, head_dim), F32),
                pltpu.VMEM((shares, per_share, model), F32),
                dma((4,)), dma((QKV_CHUNKS,)), dma((shares,)), dma((shares,)), dma((shares,)), dma((shares,)), dma((2,)),
            ],
            compiler_params=pltpu.CompilerParams(vmem_limit_bytes=VMEM_LIMIT),
            name='attend',
        )(positions, hidden, norm_attn[None, :], freq, w_qkv, k_cache.reshape(flat), v_cache.reshape(flat))

        units = w_down.shape[0]
        n_chip = n_sp // 2
        half_rows, group_rows, half = rows // 2, 2 * per_share, model // 2
        result = pl.pallas_call(
            functools.partial(tail_kernel, n_tp, n_sp),
            out_shape=jax.ShapeDtypeStruct((rows, model), BF16),
            in_specs=[vmem(), hbm(), vmem(), hbm(), hbm(), hbm()],
            out_specs=vmem(),
            scratch_shapes=[
                pltpu.VMEM(w_out.shape, BF16),
                pltpu.VMEM((model, 2 * units // n_chip), BF16),
                pltpu.VMEM((units, half), BF16),
                pltpu.VMEM((per_share, model), F32),
                pltpu.VMEM((n_sp, per_share + 1, heads, head_dim), F32),
                pltpu.VMEM((per_share * heads, head_dim), F32),
                pltpu.VMEM((CHUNKS, n_tp, per_share, model // CHUNKS), F32),
                pltpu.VMEM((CHUNKS, n_chip, per_share, model // CHUNKS), F32),
                pltpu.VMEM((half_rows, model), F32),
                pltpu.VMEM((half_rows, model), BF16),
                pltpu.VMEM((half_rows // group_rows, group_rows, units // n_chip), F32),
                pltpu.VMEM((n_chip, group_rows, units // n_chip), F32),
                pltpu.VMEM((CHUNKS, n_tp, group_rows, half // CHUNKS), F32),
                pltpu.VMEM((CHUNKS, n_sp, group_rows, half // CHUNKS), F32),
                dma((7,)),
                dma((n_sp - 1,)), dma((n_sp - 1,)),
                dma((CHUNKS, n_tp - 1)), dma((CHUNKS, n_tp - 1)),
                dma((CHUNKS, n_chip - 1)), dma((CHUNKS, n_chip - 1)),
                dma((2, n_chip - 1)), dma((2, n_chip - 1)),
                dma((CHUNKS, n_tp - 1)), dma((CHUNKS, n_tp - 1)),
                dma((CHUNKS, n_sp - 1)), dma((CHUNKS, n_sp - 1)),
            ],
            compiler_params=pltpu.CompilerParams(vmem_limit_bytes=VMEM_LIMIT, collective_id=0, has_side_effects=True),
            name='tail',
        )(parts, resid, norm_mlp[None, :], w_out, w_gate_up, w_down)
        return result, k_upd.reshape(k_cache.shape), v_upd.reshape(v_cache.shape)

    return jax.shard_map(local_step, mesh=mesh, in_specs=(P('dp', None), P('dp'), P(None), P(None), P(None, 'tp'), P('tp', None), P(None, 'tp'), P('tp', None), cache_spec, cache_spec), out_specs=(P('dp', None), cache_spec, cache_spec), check_vma=False)
```

```python
import functools

import jax
import jax.numpy as jnp
import numpy as np
from jax import lax
from jax.experimental import pallas as pl
from jax.experimental.pallas import tpu as pltpu
from jax.sharding import PartitionSpec as P

WINDOW = 2047
ROPE_BASE = 10000.0
NORM_EPS = 1e-5
MESH = pl.DeviceIdType.MESH
LANES = 128
QKV_CHUNKS = 4
CHUNKS = 4
GU_SPLITS = 2
VMEM_LIMIT = 60 * 1024 * 1024
F32, BF16 = jnp.float32, jnp.bfloat16


def dot(lhs, rhs):
    return jnp.dot(lhs, rhs, preferred_element_type=F32)


def dot_t(lhs, rhs):
    return lax.dot_general(lhs, rhs, (((1,), (1,)), ((), ())), preferred_element_type=F32)


def round_bf16(values):
    return values.astype(BF16).astype(F32)


def row_scale(values):
    return lax.rsqrt(jnp.mean(values * values, axis=-1, keepdims=True) + NORM_EPS)


def attend_kernel(dims, pos_hbm, hid_hbm, gain_hbm, freq_hbm, w_hbm, k_hbm, v_hbm, ko_hbm, vo_hbm, part_hbm, resid_hbm,
                  pos_ref, hid_ref, gain_ref, freq_ref, w_buf, k_buf, v_buf, norm_buf, proj_buf, q_buf, new_buf, s_buf,
                  part_ref, resid_ref, in_sem, w_sem, k_sem, v_sem, ko_sem, vo_sem, out_sem):
    rows, block_len, kv_count, group, shares = dims
    heads = kv_count * group
    per_share = rows // shares
    w_rows = w_buf.shape[0] // QKV_CHUNKS

    def w_copy(c):
        part = pl.ds(c * w_rows, w_rows)
        return pltpu.make_async_copy(w_hbm.at[part], w_buf.at[part], w_sem.at[c])

    def cache_copy(src, dst, sem, g):
        part = pl.ds(g * per_share, per_share)
        return pltpu.make_async_copy(src.at[part], dst.at[part], sem.at[g])

    small = [pltpu.make_async_copy(src, dst, in_sem.at[n]) for n, (src, dst) in enumerate(
        [(hid_hbm, hid_ref), (gain_hbm, gain_ref), (freq_hbm, freq_ref), (pos_hbm, pos_ref)])]
    for copy in small:
        copy.start()
    for c in range(QKV_CHUNKS):
        w_copy(c).start()
    for g in range(shares):
        cache_copy(k_hbm, k_buf, k_sem, g).start()
    for copy in small:
        copy.wait()

    resid = hid_ref[...].astype(F32)
    for n in range(resid_ref.shape[0]):
        resid_ref[n] = resid[n * 2 * per_share:(n + 1) * 2 * per_share]
    resid_copy = pltpu.make_async_copy(resid_ref, resid_hbm, out_sem.at[0])
    resid_copy.start()
    norm_buf[...] = (resid * row_scale(resid) * gain_ref[...]).astype(BF16)

    row_id = lax.broadcasted_iota(jnp.int32, (8, LANES), 0)
    tiles = []
    for r in range(rows // 8):
        tile = jnp.zeros((8, LANES), jnp.int32)
        for i in range(8):
            tile = jnp.where(row_id == i, pos_ref[r * 8 + i], tile)
        tiles.append(tile)
    angles = jnp.concatenate(tiles, axis=0).astype(F32) * freq_ref[...]
    cos_tab = jnp.cos(angles)
    sin_tab = jnp.sin(angles)
    lane_id = lax.broadcasted_iota(jnp.int32, (rows, LANES), 1)
    sin_tab = jnp.where(lane_id < LANES // 2, -sin_tab, sin_tab)

    def rope(values):
        return values * cos_tab + pltpu.roll(values, LANES // 2, axis=1) * sin_tab

    for c in range(QKV_CHUNKS):
        part = slice(c * w_rows, (c + 1) * w_rows)
        w_copy(c).wait()
        if c == QKV_CHUNKS - 1:
            for g in range(shares):
                cache_copy(v_hbm, v_buf, v_sem, g).start()
        term = dot(norm_buf[:, part], w_buf[part, :])
        proj_buf[...] = term if c == 0 else proj_buf[...] + term

    for kv in range(kv_count):
        base = kv * (group + 2) * LANES
        for g in range(group):
            q_new = round_bf16(rope(proj_buf[:, base + g * LANES:base + (g + 1) * LANES]))
            q_buf[pl.ds(kv * group + g, rows, stride=heads), :] = q_new
        k_col = base + group * LANES
        new_buf[pl.ds(kv, rows, stride=8), :] = round_bf16(rope(proj_buf[:, k_col:k_col + LANES]))
        new_buf[pl.ds(kv_count + kv, rows, stride=8), :] = round_bf16(proj_buf[:, k_col + LANES:k_col + 2 * LANES])

    start = lax.axis_index('sp') * block_len
    score_scale = LANES ** -0.5
    tile_rows = 8 * kv_count
    tile_id = lax.broadcasted_iota(jnp.int32, (tile_rows, LANES), 0)
    col_id = lax.broadcasted_iota(jnp.int32, (heads, block_len * kv_count), 1)
    head_id = lax.broadcasted_iota(jnp.int32, (heads, block_len * kv_count), 0)
    own_kv = lax.rem(col_id, kv_count) == head_id // group
    slot_id = jnp.where(own_kv, start + col_id // kv_count, -1)
    stat_lane = lax.broadcasted_iota(jnp.int32, (heads, LANES), 1)

    def write_row(buf, b, first):
        slot = pos_ref[b] - start

        @pl.when(jnp.logical_and(slot >= 0, slot < block_len))
        def _():
            base = pl.multiple_of((slot // 8) * tile_rows, tile_rows)
            tile = buf[b, pl.ds(base, tile_rows), :].astype(F32)
            lines = new_buf[pl.ds(pl.multiple_of(b * 8, 8), 8), :]
            new = jnp.zeros((tile_rows, LANES), F32)
            for kv in range(kv_count):
                line = lines[first + kv:first + kv + 1, :]
                new = jnp.where(lax.rem(tile_id, kv_count) == kv, line, new)
            hit = tile_id // kv_count == lax.rem(slot, 8)
            buf[b, pl.ds(base, tile_rows), :] = jnp.where(hit, new, tile).astype(BF16)

    def key_step(g, carry):
        cache_copy(k_hbm, k_buf, k_sem, g).wait()
        for i in range(per_share):
            write_row(k_buf, g * per_share + i, 0)
        cache_copy(k_buf, ko_hbm, ko_sem, g).start()
        for i in range(per_share):
            b = g * per_share + i
            q_rows = q_buf[pl.ds(pl.multiple_of(b * heads, heads), heads), :].astype(BF16)
            s_buf[b] = dot_t(q_rows, k_buf[b])
        return carry

    def weight_step(g, carry):
        stats = jnp.zeros((heads, LANES), F32)
        for i in range(per_share):
            b = g * per_share + i
            pos = pos_ref[b]
            seen = (slot_id <= pos) & (slot_id >= jnp.maximum(pos - WINDOW, 0))
            scores = jnp.where(seen, s_buf[b] * score_scale, -jnp.inf)
            top = jnp.max(scores, axis=-1, keepdims=True)
            base = jnp.where(top == -jnp.inf, 0.0, top)
            weights = jnp.exp(scores - base)
            total = jnp.sum(weights, axis=-1, keepdims=True)
            s_buf[b] = weights
            stats = jnp.where(stat_lane == i, top, stats)
            stats = jnp.where(stat_lane == per_share + i, total, stats)
        part_ref[g, per_share] = stats
        return carry

    def value_step(g, carry):
        cache_copy(v_hbm, v_buf, v_sem, g).wait()
        for i in range(per_share):
            write_row(v_buf, g * per_share + i, kv_count)
        cache_copy(v_buf, vo_hbm, vo_sem, g).start()
        for i in range(per_share):
            b = g * per_share + i
            part_ref[g, i] = dot(s_buf[b].astype(BF16), v_buf[b])
        return carry

    lax.fori_loop(0, shares, key_step, 0)
    lax.fori_loop(0, shares, weight_step, 0)
    lax.fori_loop(0, shares, value_step, 0)
    part_copy = pltpu.make_async_copy(part_ref, part_hbm, out_sem.at[1])
    part_copy.start()
    for g in range(shares):
        cache_copy(k_buf, ko_hbm, ko_sem, g).wait()
        cache_copy(v_buf, vo_hbm, vo_sem, g).wait()
    resid_copy.wait()
    part_copy.wait()


def tail_kernel(n_tp, n_sp, part_ref, resid_hbm, gain_ref, wo_hbm, wgu_hbm, wd_hbm, out_ref,
                wo_buf, wgu_buf, wd_own, wd_mate, resid_buf, part_in, att_buf, y1_buf, x1_in, r2_buf,
                z_out, z_in, y2_buf, x2_in, w_sem, b_send, b_recv, m_send, m_recv, y1_send, y1_recv,
                y2_send, y2_recv, g2_send, g2_recv):
    t = lax.axis_index('tp')
    s = lax.axis_index('sp')
    n_chip = n_sp // 2
    chip, core = s // 2, lax.rem(s, 2)
    other = 1 - core
    mate = chip * 2 + other
    units, model = wd_hbm.shape
    core_units = units // 2
    split = core_units // GU_SPLITS
    half = model // 2
    width = half // CHUNKS
    per_share = part_ref.shape[1] - 1
    heads = part_ref.shape[2]
    share_rows = per_share * heads
    rows = 2 * per_share

    def columns(which, size):
        return pl.ds(pl.multiple_of(which * size, LANES), size)

    resid_load = pltpu.make_async_copy(resid_hbm.at[chip, :, columns(core, half)], resid_buf, w_sem.at[0])
    wo_load = pltpu.make_async_copy(wo_hbm.at[:, columns(core, half)], wo_buf, w_sem.at[1])
    gu_loads = []
    for n in range(GU_SPLITS):
        for side in range(2):
            col = pl.multiple_of(side * units + core * core_units + n * split, LANES)
            at = (2 * n + side) * split
            gu_loads.append(pltpu.make_async_copy(wgu_hbm.at[:, pl.ds(col, split)], wgu_buf.at[:, pl.ds(at, split)], w_sem.at[4 + len(gu_loads)]))
    wd_rows = columns(core, core_units)
    wd_loads = [
        pltpu.make_async_copy(wd_hbm.at[wd_rows, columns(other, half)], wd_mate, w_sem.at[2]),
        pltpu.make_async_copy(wd_hbm.at[wd_rows, columns(core, half)], wd_own, w_sem.at[3]),
    ]
    resid_load.start()
    wo_load.start()

    def wrap(value, count):
        return lax.rem(value + count, count)

    barrier = pltpu.get_barrier_semaphore()
    for k in range(1, n_sp):
        pl.semaphore_signal(barrier, inc=1, device_id={'sp': wrap(s + k, n_sp)}, device_id_type=MESH)
    for k in range(1, n_tp):
        pl.semaphore_signal(barrier, inc=1, device_id={'tp': wrap(t + k, n_tp)}, device_id_type=MESH)
    pl.semaphore_wait(barrier, n_sp + n_tp - 2)

    sent = []

    def push(src, dst, send, recv, device):
        copy = pltpu.make_async_remote_copy(src_ref=src, dst_ref=dst, send_sem=send, recv_sem=recv, device_id=device, device_id_type=MESH)
        copy.start()
        sent.append(copy)

    def arrive(dst, recv):
        pltpu.make_async_remote_copy(src_ref=dst, dst_ref=dst, send_sem=b_send.at[0], recv_sem=recv, device_id={'sp': mate}, device_id_type=MESH).wait_recv()

    to_mate = {'sp': mate}
    near_first = sorted(range(1, n_chip), key=lambda k: min(k, n_chip - k))
    far_first = near_first[::-1]

    for k in range(1, n_sp):
        dev = wrap(s + k, n_sp)
        push(part_ref.at[dev], part_in.at[s], b_send.at[k - 1], b_recv.at[k - 1], {'sp': dev})
    part_in[s] = part_ref[s]
    resid_load.wait()
    wo_load.wait()
    for load in gu_loads[:2]:
        load.start()
    for k in range(1, n_sp):
        arrive(part_in.at[wrap(s - k, n_sp)], b_recv.at[k - 1])
    stats = [part_in[j, per_share] for j in range(n_sp)]
    top = functools.reduce(jnp.maximum, stats)
    scales = [jnp.exp(st - top) for st in stats]
    total = sum(sc * pltpu.roll(st, LANES - per_share, axis=1) for sc, st in zip(scales, stats))
    for i in range(per_share):
        acc = sum(part_in[j, i] * scales[j][:, i:i + 1] for j in range(n_sp))
        at = pl.multiple_of(core * share_rows + i * heads, heads)
        att_buf[pl.ds(at, heads), :] = round_bf16(acc / total[:, i:i + 1])
    mine = att_buf.at[pl.ds(pl.multiple_of(core * share_rows, heads), share_rows)]
    push(mine, mine, m_send.at[0], m_recv.at[0], to_mate)
    for load in gu_loads[2:]:
        load.start()
    arrive(att_buf.at[pl.ds(pl.multiple_of(other * share_rows, heads), share_rows)], m_recv.at[0])
    attended = jnp.concatenate([att_buf[pl.ds(h, rows, stride=heads), :] for h in range(heads)], axis=1).astype(BF16)

    for n in range(CHUNKS):
        y1_buf[n, t] = round_bf16(dot(attended, wo_buf[:, n * width:(n + 1) * width]))
        for k in range(1, n_tp):
            push(y1_buf.at[n, t], y1_buf.at[n, t], y1_send.at[n, k - 1], y1_recv.at[n, k - 1], {'tp': wrap(t + k, n_tp)})
    for load in wd_loads:
        load.start()
    for n in range(CHUNKS):
        for k in range(1, n_tp):
            arrive(y1_buf.at[n, wrap(t - k, n_tp)], y1_recv.at[n, k - 1])
        out_sum = functools.reduce(jnp.add, [y1_buf[n, j] for j in range(n_tp)])
        x1_in[core, n] = resid_buf[:, n * width:(n + 1) * width] + out_sum
        push(x1_in.at[core, n], x1_in.at[core, n], m_send.at[1 + n], m_recv.at[1 + n], to_mate)
    square = jnp.zeros((rows, LANES), F32)
    for n in range(CHUNKS):
        arrive(x1_in.at[other, n], m_recv.at[1 + n])
        for c in range(2):
            for at in range(0, width, LANES):
                piece = x1_in[c, n, :, at:at + LANES]
                square = square + piece * piece
    scale = lax.rsqrt(jnp.sum(square, axis=-1, keepdims=True) / model + NORM_EPS)
    for c in range(2):
        for n in range(CHUNKS):
            part = slice(c * half + n * width, c * half + (n + 1) * width)
            r2_buf[:, part] = (x1_in[c, n] * scale * gain_ref[:, part]).astype(BF16)

    acts = []
    for n in range(GU_SPLITS):
        gu_loads[2 * n].wait()
        gu_loads[2 * n + 1].wait()
        both = dot(r2_buf[...], wgu_buf[:, 2 * n * split:2 * (n + 1) * split])
        gate = both[:, :split]
        acts.append((gate * jax.nn.sigmoid(gate) * both[:, split:]).astype(BF16))
    act = jnp.concatenate(acts, axis=1)
    wd_loads[0].wait()
    for n in range(CHUNKS):
        z_out[n] = dot(act, wd_mate[:, n * width:(n + 1) * width])
        push(z_out.at[n], z_in.at[n], m_send.at[1 + CHUNKS + n], m_recv.at[1 + CHUNKS + n], to_mate)
    wd_loads[1].wait()
    for n in range(CHUNKS):
        own = dot(act, wd_own[:, n * width:(n + 1) * width])
        arrive(z_in.at[n], m_recv.at[1 + CHUNKS + n])
        y2_buf[n, t] = round_bf16(own + z_in[n])
        for k in range(1, n_tp):
            push(y2_buf.at[n, t], y2_buf.at[n, t], y2_send.at[n, k - 1], y2_recv.at[n, k - 1], {'tp': wrap(t + k, n_tp)})
    for n in range(CHUNKS):
        for k in range(1, n_tp):
            arrive(y2_buf.at[n, wrap(t - k, n_tp)], y2_recv.at[n, k - 1])
        down_sum = functools.reduce(jnp.add, [y2_buf[n, j] for j in range(n_tp)])
        x2_in[n, s] = x1_in[core, n] + down_sum
        for k in far_first:
            push(x2_in.at[n, s], x2_in.at[n, s], g2_send.at[n, k], g2_recv.at[n, k], {'sp': wrap(chip + k, n_chip) * 2 + core})
        push(x2_in.at[n, s], x2_in.at[n, s], g2_send.at[n, 0], g2_recv.at[n, 0], to_mate)
    for n in range(CHUNKS):
        for k in near_first:
            far = x2_in.at[n, wrap(chip - k, n_chip) * 2 + core]
            arrive(far, g2_recv.at[n, k])
            push(far, far, g2_send.at[n, n_chip + k - 1], g2_recv.at[n, n_chip + k - 1], to_mate)
    for n in range(CHUNKS):
        arrive(x2_in.at[n, mate], g2_recv.at[n, 0])
        for k in near_first:
            arrive(x2_in.at[n, wrap(chip - k, n_chip) * 2 + other], g2_recv.at[n, n_chip + k - 1])
        for j in range(0, n_chip, 2):
            for c in range(2):
                lines = jnp.concatenate([x2_in[n, 2 * j + c], x2_in[n, 2 * j + 2 + c]], axis=0)
                col = c * half + n * width
                out_ref[j * rows:(j + 2) * rows, col:col + width] = lines.astype(BF16)
    for copy in sent:
        copy.wait_send()


def vmem():
    return pl.BlockSpec(memory_space=pltpu.VMEM)


def hbm():
    return pl.BlockSpec(memory_space=pl.ANY)


def solution(mesh):
    n_tp, n_sp = mesh.shape['tp'], mesh.shape['sp']
    cache_spec = P('dp', 'sp', 'tp', None)

    def local_step(hidden, positions, norm_attn, norm_mlp, w_qkv, w_out, w_gate_up, w_down, k_cache, v_cache):
        rows, block_len, kv_count, head_dim = k_cache.shape
        model = hidden.shape[1]
        group = w_qkv.shape[1] // (kv_count * head_dim) - 2
        heads = kv_count * group
        shares = n_sp
        per_share = rows // shares
        flat = (rows, block_len * kv_count, head_dim)
        inv_freq = ROPE_BASE ** (-np.arange(0, head_dim, 2) / head_dim)
        freq = jnp.asarray(np.concatenate([inv_freq, inv_freq])[None, :], F32)
        dma = pltpu.SemaphoreType.DMA

        k_upd, v_upd, parts, resid = pl.pallas_call(
            functools.partial(attend_kernel, (rows, block_len, kv_count, group, shares)),
            out_shape=(
                jax.ShapeDtypeStruct(flat, BF16),
                jax.ShapeDtypeStruct(flat, BF16),
                jax.ShapeDtypeStruct((shares, per_share + 1, heads, head_dim), F32),
                jax.ShapeDtypeStruct((shares // 2, 2 * per_share, model), F32),
            ),
            in_specs=[hbm()] * 7,
            out_specs=(hbm(), hbm(), hbm(), hbm()),
            scratch_shapes=[
                pltpu.SMEM(positions.shape, jnp.int32),
                pltpu.VMEM(hidden.shape, BF16),
                pltpu.VMEM((1, model), F32),
                pltpu.VMEM(freq.shape, F32),
                pltpu.VMEM(w_qkv.shape, BF16),
                pltpu.VMEM(flat, BF16),
                pltpu.VMEM(flat, BF16),
                pltpu.VMEM((rows, model), BF16),
                pltpu.VMEM((rows, w_qkv.shape[1]), F32),
                pltpu.VMEM((rows * heads, head_dim), F32),
                pltpu.VMEM((rows * 8, head_dim), F32),
                pltpu.VMEM((rows, heads, block_len * kv_count), F32),
                pltpu.VMEM((shares, per_share + 1, heads, head_dim), F32),
                pltpu.VMEM((shares // 2, 2 * per_share, model), F32),
                dma((4,)), dma((QKV_CHUNKS,)), dma((shares,)), dma((shares,)), dma((shares,)), dma((shares,)), dma((2,)),
            ],
            compiler_params=pltpu.CompilerParams(vmem_limit_bytes=VMEM_LIMIT),
            name='attend',
        )(positions, hidden, norm_attn[None, :], freq, w_qkv, k_cache.reshape(flat), v_cache.reshape(flat))

        units = w_down.shape[0]
        chip_rows, half = 2 * per_share, model // 2
        result = pl.pallas_call(
            functools.partial(tail_kernel, n_tp, n_sp),
            out_shape=jax.ShapeDtypeStruct((rows, model), BF16),
            in_specs=[vmem(), hbm(), vmem(), hbm(), hbm(), hbm()],
            out_specs=vmem(),
            scratch_shapes=[
                pltpu.VMEM((w_out.shape[0], half), BF16),
                pltpu.VMEM((model, units), BF16),
                pltpu.VMEM((units // 2, half), BF16),
                pltpu.VMEM((units // 2, half), BF16),
                pltpu.VMEM((chip_rows, half), F32),
                pltpu.VMEM((n_sp, per_share + 1, heads, head_dim), F32),
                pltpu.VMEM((chip_rows * heads, head_dim), F32),
                pltpu.VMEM((CHUNKS, n_tp, chip_rows, half // CHUNKS), F32),
                pltpu.VMEM((2, CHUNKS, chip_rows, half // CHUNKS), F32),
                pltpu.VMEM((chip_rows, model), BF16),
                pltpu.VMEM((CHUNKS, chip_rows, half // CHUNKS), F32),
                pltpu.VMEM((CHUNKS, chip_rows, half // CHUNKS), F32),
                pltpu.VMEM((CHUNKS, n_tp, chip_rows, half // CHUNKS), F32),
                pltpu.VMEM((CHUNKS, n_sp, chip_rows, half // CHUNKS), F32),
                dma((4 + 2 * GU_SPLITS,)),
                dma((n_sp - 1,)), dma((n_sp - 1,)),
                dma((1 + 2 * CHUNKS,)), dma((1 + 2 * CHUNKS,)),
                dma((CHUNKS, n_tp - 1)), dma((CHUNKS, n_tp - 1)),
                dma((CHUNKS, n_tp - 1)), dma((CHUNKS, n_tp - 1)),
                dma((CHUNKS, n_sp - 1)), dma((CHUNKS, n_sp - 1)),
            ],
            compiler_params=pltpu.CompilerParams(vmem_limit_bytes=VMEM_LIMIT, collective_id=0, has_side_effects=True),
            name='tail',
        )(parts, resid, norm_mlp[None, :], w_out, w_gate_up, w_down)
        return result, k_upd.reshape(k_cache.shape), v_upd.reshape(v_cache.shape)

    return jax.shard_map(local_step, mesh=mesh, in_specs=(P('dp', None), P('dp'), P(None), P(None), P(None, 'tp'), P('tp', None), P(None, 'tp'), P('tp', None), cache_spec, cache_spec), out_specs=(P('dp', None), cache_spec, cache_spec), check_vma=False)
```

```python
import functools

import jax
import jax.numpy as jnp
import numpy as np
from jax import lax
from jax.experimental import pallas as pl
from jax.experimental.pallas import tpu as pltpu
from jax.sharding import PartitionSpec as P

WINDOW = 2047
ROPE_BASE = 10000.0
NORM_EPS = 1e-5
MESH = pl.DeviceIdType.MESH
LANES = 128
QKV_CHUNKS = 4
OUT_CHUNKS = 2
DOWN_CHUNKS = 2
GU_SPLITS = 2
ATTEND_VMEM = 60 * 1024 * 1024
TAIL_VMEM = 52 * 1024 * 1024
F32, BF16 = jnp.float32, jnp.bfloat16


def dot(lhs, rhs):
    return jnp.dot(lhs, rhs, preferred_element_type=F32)


def dot_t(lhs, rhs):
    return lax.dot_general(lhs, rhs, (((1,), (1,)), ((), ())), preferred_element_type=F32)


def round_bf16(values):
    return values.astype(BF16).astype(F32)


def row_scale(values):
    return lax.rsqrt(jnp.mean(values * values, axis=-1, keepdims=True) + NORM_EPS)


def attend_kernel(dims, pos_hbm, hid_hbm, gain_hbm, freq_hbm, w_hbm, k_hbm, v_hbm, ko_hbm, vo_hbm, part_hbm, resid_hbm,
                  pos_ref, hid_ref, gain_ref, freq_ref, w_buf, k_buf, v_buf, norm_buf, proj_buf, q_buf, new_buf, s_buf,
                  part_ref, resid_ref, in_sem, w_sem, k_sem, v_sem, ko_sem, vo_sem, out_sem):
    rows, block_len, kv_count, group, shares = dims
    heads = kv_count * group
    per_share = rows // shares
    w_rows = w_buf.shape[0] // QKV_CHUNKS

    def w_copy(c):
        part = pl.ds(c * w_rows, w_rows)
        return pltpu.make_async_copy(w_hbm.at[part], w_buf.at[part], w_sem.at[c])

    def cache_copy(src, dst, sem, g):
        part = pl.ds(g * per_share, per_share)
        return pltpu.make_async_copy(src.at[part], dst.at[part], sem.at[g])

    small = [pltpu.make_async_copy(src, dst, in_sem.at[n]) for n, (src, dst) in enumerate(
        [(hid_hbm, hid_ref), (gain_hbm, gain_ref), (freq_hbm, freq_ref), (pos_hbm, pos_ref)])]
    for copy in small:
        copy.start()
    for c in range(QKV_CHUNKS):
        w_copy(c).start()
    for g in range(shares):
        cache_copy(k_hbm, k_buf, k_sem, g).start()
    for copy in small:
        copy.wait()

    resid = hid_ref[...].astype(F32)
    for n in range(resid_ref.shape[0]):
        resid_ref[n] = resid[n * 2 * per_share:(n + 1) * 2 * per_share]
    resid_copy = pltpu.make_async_copy(resid_ref, resid_hbm, out_sem.at[0])
    resid_copy.start()
    norm_buf[...] = (resid * row_scale(resid) * gain_ref[...]).astype(BF16)

    row_id = lax.broadcasted_iota(jnp.int32, (8, LANES), 0)
    tiles = []
    for r in range(rows // 8):
        tile = jnp.zeros((8, LANES), jnp.int32)
        for i in range(8):
            tile = jnp.where(row_id == i, pos_ref[r * 8 + i], tile)
        tiles.append(tile)
    angles = jnp.concatenate(tiles, axis=0).astype(F32) * freq_ref[...]
    cos_tab = jnp.cos(angles)
    sin_tab = jnp.sin(angles)
    lane_id = lax.broadcasted_iota(jnp.int32, (rows, LANES), 1)
    sin_tab = jnp.where(lane_id < LANES // 2, -sin_tab, sin_tab)

    def rope(values):
        return values * cos_tab + pltpu.roll(values, LANES // 2, axis=1) * sin_tab

    for c in range(QKV_CHUNKS):
        part = slice(c * w_rows, (c + 1) * w_rows)
        w_copy(c).wait()
        if c == QKV_CHUNKS - 1:
            for g in range(shares):
                cache_copy(v_hbm, v_buf, v_sem, g).start()
        term = dot(norm_buf[:, part], w_buf[part, :])
        proj_buf[...] = term if c == 0 else proj_buf[...] + term

    for kv in range(kv_count):
        base = kv * (group + 2) * LANES
        for g in range(group):
            q_new = round_bf16(rope(proj_buf[:, base + g * LANES:base + (g + 1) * LANES]))
            q_buf[pl.ds(kv * group + g, rows, stride=heads), :] = q_new
        k_col = base + group * LANES
        new_buf[pl.ds(kv, rows, stride=8), :] = round_bf16(rope(proj_buf[:, k_col:k_col + LANES]))
        new_buf[pl.ds(kv_count + kv, rows, stride=8), :] = round_bf16(proj_buf[:, k_col + LANES:k_col + 2 * LANES])

    start = lax.axis_index('sp') * block_len
    score_scale = LANES ** -0.5
    tile_rows = 8 * kv_count
    tile_id = lax.broadcasted_iota(jnp.int32, (tile_rows, LANES), 0)
    col_id = lax.broadcasted_iota(jnp.int32, (heads, block_len * kv_count), 1)
    head_id = lax.broadcasted_iota(jnp.int32, (heads, block_len * kv_count), 0)
    own_kv = lax.rem(col_id, kv_count) == head_id // group
    slot_id = jnp.where(own_kv, start + col_id // kv_count, -1)
    stat_lane = lax.broadcasted_iota(jnp.int32, (heads, LANES), 1)

    def write_row(buf, b, first):
        slot = pos_ref[b] - start

        @pl.when(jnp.logical_and(slot >= 0, slot < block_len))
        def _():
            base = pl.multiple_of((slot // 8) * tile_rows, tile_rows)
            tile = buf[b, pl.ds(base, tile_rows), :].astype(F32)
            lines = new_buf[pl.ds(pl.multiple_of(b * 8, 8), 8), :]
            new = jnp.zeros((tile_rows, LANES), F32)
            for kv in range(kv_count):
                line = lines[first + kv:first + kv + 1, :]
                new = jnp.where(lax.rem(tile_id, kv_count) == kv, line, new)
            hit = tile_id // kv_count == lax.rem(slot, 8)
            buf[b, pl.ds(base, tile_rows), :] = jnp.where(hit, new, tile).astype(BF16)

    def key_step(g, carry):
        cache_copy(k_hbm, k_buf, k_sem, g).wait()
        for i in range(per_share):
            write_row(k_buf, g * per_share + i, 0)
        cache_copy(k_buf, ko_hbm, ko_sem, g).start()
        for i in range(per_share):
            b = g * per_share + i
            q_rows = q_buf[pl.ds(pl.multiple_of(b * heads, heads), heads), :].astype(BF16)
            s_buf[b] = dot_t(q_rows, k_buf[b])
        return carry

    def weight_step(g, carry):
        stats = jnp.zeros((heads, LANES), F32)
        for i in range(per_share):
            b = g * per_share + i
            pos = pos_ref[b]
            seen = (slot_id <= pos) & (slot_id >= jnp.maximum(pos - WINDOW, 0))
            scores = jnp.where(seen, s_buf[b] * score_scale, -jnp.inf)
            top = jnp.max(scores, axis=-1, keepdims=True)
            base = jnp.where(top == -jnp.inf, 0.0, top)
            weights = jnp.exp(scores - base)
            total = jnp.sum(weights, axis=-1, keepdims=True)
            s_buf[b] = weights
            stats = jnp.where(stat_lane == i, top, stats)
            stats = jnp.where(stat_lane == per_share + i, total, stats)
        part_ref[g, per_share] = stats
        return carry

    def value_step(g, carry):
        cache_copy(v_hbm, v_buf, v_sem, g).wait()
        for i in range(per_share):
            write_row(v_buf, g * per_share + i, kv_count)
        cache_copy(v_buf, vo_hbm, vo_sem, g).start()
        for i in range(per_share):
            b = g * per_share + i
            part_ref[g, i] = dot(s_buf[b].astype(BF16), v_buf[b])
        return carry

    lax.fori_loop(0, shares, key_step, 0)
    lax.fori_loop(0, shares, weight_step, 0)
    lax.fori_loop(0, shares, value_step, 0)
    part_copy = pltpu.make_async_copy(part_ref, part_hbm, out_sem.at[1])
    part_copy.start()
    for g in range(shares):
        cache_copy(k_buf, ko_hbm, ko_sem, g).wait()
        cache_copy(v_buf, vo_hbm, vo_sem, g).wait()
    resid_copy.wait()
    part_copy.wait()


def tail_kernel(n_tp, n_sp, part_hbm, resid_hbm, gain_hbm, wo_hbm, wgu_hbm, wd_hbm, out_ref,
                gain_ref, wo_buf, wgu_buf, wd_own, wd_mate, resid_buf, part_in, att_buf, y1_buf, x1_own, r2_buf,
                z_out, z_in, y2_buf, x2_in, w_sem, b_send, b_recv, m_send, m_recv, y1_send, y1_recv,
                y2_send, y2_recv, g2_send, g2_recv):
    t = lax.axis_index('tp')
    s = lax.axis_index('sp')
    n_chip = n_sp // 2
    chip, core = s // 2, lax.rem(s, 2)
    other = 1 - core
    mate = chip * 2 + other
    units, model = wd_hbm.shape
    core_units = units // 2
    split = core_units // GU_SPLITS
    half = model // 2
    width = half // OUT_CHUNKS
    down_width = half // DOWN_CHUNKS
    per_share = part_hbm.shape[1] - 1
    heads = part_hbm.shape[2]
    share_rows = per_share * heads
    rows = 2 * per_share

    def columns(which, size):
        return pl.ds(pl.multiple_of(which * size, LANES), size)

    resid_load = pltpu.make_async_copy(resid_hbm.at[chip, :, columns(core, half)], resid_buf, w_sem.at[0])
    wo_load = pltpu.make_async_copy(wo_hbm.at[:, columns(core, half)], wo_buf, w_sem.at[1])
    gu_loads = []
    for n in range(GU_SPLITS):
        for side in range(2):
            col = pl.multiple_of(side * units + core * core_units + n * split, LANES)
            at = (2 * n + side) * split
            gu_loads.append(pltpu.make_async_copy(wgu_hbm.at[:, pl.ds(col, split)], wgu_buf.at[:, pl.ds(at, split)], w_sem.at[4 + len(gu_loads)]))
    wd_rows = columns(core, core_units)
    wd_loads = [
        pltpu.make_async_copy(wd_hbm.at[wd_rows, columns(other, half)], wd_mate, w_sem.at[2]),
        pltpu.make_async_copy(wd_hbm.at[wd_rows, columns(core, half)], wd_own, w_sem.at[3]),
    ]
    part_load = pltpu.make_async_copy(part_hbm.at[s], part_in.at[s], w_sem.at[4 + 2 * GU_SPLITS])
    gain_load = pltpu.make_async_copy(gain_hbm, gain_ref, w_sem.at[5 + 2 * GU_SPLITS])
    part_load.start()

    def wrap(value, count):
        return lax.rem(value + count, count)

    barrier = pltpu.get_barrier_semaphore()
    for k in range(1, n_sp):
        pl.semaphore_signal(barrier, inc=1, device_id={'sp': wrap(s + k, n_sp)}, device_id_type=MESH)
    for k in range(1, n_tp):
        pl.semaphore_signal(barrier, inc=1, device_id={'tp': wrap(t + k, n_tp)}, device_id_type=MESH)
    resid_load.start()
    gain_load.start()
    pl.semaphore_wait(barrier, n_sp + n_tp - 2)

    sent = []

    def push(src, dst, send, recv, device):
        copy = pltpu.make_async_remote_copy(src_ref=src, dst_ref=dst, send_sem=send, recv_sem=recv, device_id=device, device_id_type=MESH)
        copy.start()
        sent.append(copy)

    def arrive(dst, recv):
        pltpu.make_async_remote_copy(src_ref=dst, dst_ref=dst, send_sem=b_send.at[0], recv_sem=recv, device_id={'sp': mate}, device_id_type=MESH).wait_recv()

    to_mate = {'sp': mate}
    near_first = sorted(range(1, n_chip), key=lambda k: min(k, n_chip - k))
    far_first = near_first[::-1]

    for k in range(1, n_sp):
        dev = wrap(s + k, n_sp)
        push(part_hbm.at[dev], part_in.at[s], b_send.at[k - 1], b_recv.at[k - 1], {'sp': dev})
    wo_load.start()
    part_load.wait()
    resid_load.wait()
    gain_load.wait()
    wo_load.wait()
    for load in gu_loads[:2]:
        load.start()
    for k in range(1, n_sp):
        arrive(part_in.at[wrap(s - k, n_sp)], b_recv.at[k - 1])
    stats = [part_in[j, per_share] for j in range(n_sp)]
    top = functools.reduce(jnp.maximum, stats)
    scales = [jnp.exp(st - top) for st in stats]
    total = sum(sc * pltpu.roll(st, LANES - per_share, axis=1) for sc, st in zip(scales, stats))
    for i in range(per_share):
        acc = sum(part_in[j, i] * scales[j][:, i:i + 1] for j in range(n_sp))
        at = pl.multiple_of(core * share_rows + i * heads, heads)
        att_buf[pl.ds(at, heads), :] = round_bf16(acc / total[:, i:i + 1])
    mine = att_buf.at[pl.ds(pl.multiple_of(core * share_rows, heads), share_rows)]
    push(mine, mine, m_send.at[0], m_recv.at[0], to_mate)
    for load in gu_loads[2:]:
        load.start()
    arrive(att_buf.at[pl.ds(pl.multiple_of(other * share_rows, heads), share_rows)], m_recv.at[0])
    attended = jnp.concatenate([att_buf[pl.ds(h, rows, stride=heads), :] for h in range(heads)], axis=1).astype(BF16)

    for n in range(OUT_CHUNKS):
        y1_buf[n, t] = round_bf16(dot(attended, wo_buf[:, n * width:(n + 1) * width]))
        for k in range(1, n_tp):
            push(y1_buf.at[n, t], y1_buf.at[n, t], y1_send.at[n, k - 1], y1_recv.at[n, k - 1], {'tp': wrap(t + k, n_tp)})
    for load in wd_loads:
        load.start()
    for n in range(OUT_CHUNKS):
        for k in range(1, n_tp):
            arrive(y1_buf.at[n, wrap(t - k, n_tp)], y1_recv.at[n, k - 1])
        out_sum = functools.reduce(jnp.add, [y1_buf[n, j] for j in range(n_tp)])
        x1_own[core, :, n * width:(n + 1) * width] = resid_buf[:, n * width:(n + 1) * width] + out_sum
        part = x1_own.at[core, :, pl.ds(n * width, width)]
        push(part, part, m_send.at[1 + n], m_recv.at[1 + n], to_mate)
    square = jnp.zeros((rows, LANES), F32)
    for n in range(OUT_CHUNKS):
        arrive(x1_own.at[other, :, pl.ds(n * width, width)], m_recv.at[1 + n])
        for c in range(2):
            for at in range(0, width, LANES):
                piece = x1_own[c, :, n * width + at:n * width + at + LANES]
                square = square + piece * piece
    scale = lax.rsqrt(jnp.sum(square, axis=-1, keepdims=True) / model + NORM_EPS)
    for c in range(2):
        for n in range(OUT_CHUNKS):
            part = slice(c * half + n * width, c * half + (n + 1) * width)
            r2_buf[:, part] = (x1_own[c, :, n * width:(n + 1) * width] * scale * gain_ref[:, part]).astype(BF16)

    acts = []
    for n in range(GU_SPLITS):
        gu_loads[2 * n].wait()
        gu_loads[2 * n + 1].wait()
        both = dot(r2_buf[...], wgu_buf[:, 2 * n * split:2 * (n + 1) * split])
        gate = both[:, :split]
        acts.append((gate * jax.nn.sigmoid(gate) * both[:, split:]).astype(BF16))
    act = jnp.concatenate(acts, axis=1)
    wd_loads[0].wait()
    for n in range(DOWN_CHUNKS):
        z_out[n] = dot(act, wd_mate[:, n * down_width:(n + 1) * down_width])
        push(z_out.at[n], z_in.at[n], m_send.at[1 + OUT_CHUNKS + n], m_recv.at[1 + OUT_CHUNKS + n], to_mate)
    wd_loads[1].wait()
    for n in range(DOWN_CHUNKS):
        own = dot(act, wd_own[:, n * down_width:(n + 1) * down_width])
        arrive(z_in.at[n], m_recv.at[1 + OUT_CHUNKS + n])
        y2_buf[n, t] = round_bf16(own + z_in[n])
        for k in range(1, n_tp):
            push(y2_buf.at[n, t], y2_buf.at[n, t], y2_send.at[n, k - 1], y2_recv.at[n, k - 1], {'tp': wrap(t + k, n_tp)})
    for n in range(DOWN_CHUNKS):
        for k in range(1, n_tp):
            arrive(y2_buf.at[n, wrap(t - k, n_tp)], y2_recv.at[n, k - 1])
        down_sum = functools.reduce(jnp.add, [y2_buf[n, j] for j in range(n_tp)])
        x2_in[n, s] = x1_own[core, :, n * down_width:(n + 1) * down_width] + down_sum
        for k in far_first:
            push(x2_in.at[n, s], x2_in.at[n, s], g2_send.at[n, k], g2_recv.at[n, k], {'sp': wrap(chip + k, n_chip) * 2 + core})
        push(x2_in.at[n, s], x2_in.at[n, s], g2_send.at[n, 0], g2_recv.at[n, 0], to_mate)
    for n in range(DOWN_CHUNKS):
        for k in near_first:
            far = x2_in.at[n, wrap(chip - k, n_chip) * 2 + core]
            arrive(far, g2_recv.at[n, k])
            push(far, far, g2_send.at[n, n_chip + k - 1], g2_recv.at[n, n_chip + k - 1], to_mate)
    for n in range(DOWN_CHUNKS):
        arrive(x2_in.at[n, mate], g2_recv.at[n, 0])
        for k in near_first:
            arrive(x2_in.at[n, wrap(chip - k, n_chip) * 2 + other], g2_recv.at[n, n_chip + k - 1])
        for j in range(0, n_chip, 2):
            for c in range(2):
                lines = jnp.concatenate([x2_in[n, 2 * j + c], x2_in[n, 2 * j + 2 + c]], axis=0)
                col = c * half + n * down_width
                out_ref[j * rows:(j + 2) * rows, col:col + down_width] = lines.astype(BF16)
    for copy in sent:
        copy.wait_send()


def vmem():
    return pl.BlockSpec(memory_space=pltpu.VMEM)


def hbm():
    return pl.BlockSpec(memory_space=pl.ANY)


def solution(mesh):
    n_tp, n_sp = mesh.shape['tp'], mesh.shape['sp']
    cache_spec = P('dp', 'sp', 'tp', None)

    def local_step(hidden, positions, norm_attn, norm_mlp, w_qkv, w_out, w_gate_up, w_down, k_cache, v_cache):
        rows, block_len, kv_count, head_dim = k_cache.shape
        model = hidden.shape[1]
        group = w_qkv.shape[1] // (kv_count * head_dim) - 2
        heads = kv_count * group
        shares = n_sp
        per_share = rows // shares
        flat = (rows, block_len * kv_count, head_dim)
        inv_freq = ROPE_BASE ** (-np.arange(0, head_dim, 2) / head_dim)
        freq = jnp.asarray(np.concatenate([inv_freq, inv_freq])[None, :], F32)
        dma = pltpu.SemaphoreType.DMA

        k_upd, v_upd, parts, resid = pl.pallas_call(
            functools.partial(attend_kernel, (rows, block_len, kv_count, group, shares)),
            out_shape=(
                jax.ShapeDtypeStruct(flat, BF16),
                jax.ShapeDtypeStruct(flat, BF16),
                pltpu.VMEM((shares, per_share + 1, heads, head_dim), F32),
                pltpu.VMEM((shares // 2, 2 * per_share, model), F32),
            ),
            in_specs=[hbm()] * 7,
            out_specs=(hbm(), hbm(), hbm(), hbm()),
            scratch_shapes=[
                pltpu.SMEM(positions.shape, jnp.int32),
                pltpu.VMEM(hidden.shape, BF16),
                pltpu.VMEM((1, model), F32),
                pltpu.VMEM(freq.shape, F32),
                pltpu.VMEM(w_qkv.shape, BF16),
                pltpu.VMEM(flat, BF16),
                pltpu.VMEM(flat, BF16),
                pltpu.VMEM((rows, model), BF16),
                pltpu.VMEM((rows, w_qkv.shape[1]), F32),
                pltpu.VMEM((rows * heads, head_dim), F32),
                pltpu.VMEM((rows * 8, head_dim), F32),
                pltpu.VMEM((rows, heads, block_len * kv_count), F32),
                pltpu.VMEM((shares, per_share + 1, heads, head_dim), F32),
                pltpu.VMEM((shares // 2, 2 * per_share, model), F32),
                dma((4,)), dma((QKV_CHUNKS,)), dma((shares,)), dma((shares,)), dma((shares,)), dma((shares,)), dma((2,)),
            ],
            compiler_params=pltpu.CompilerParams(vmem_limit_bytes=ATTEND_VMEM),
            name='attend',
        )(positions, hidden, norm_attn[None, :], freq, w_qkv, k_cache.reshape(flat), v_cache.reshape(flat))

        units = w_down.shape[0]
        chip_rows, half = 2 * per_share, model // 2
        result = pl.pallas_call(
            functools.partial(tail_kernel, n_tp, n_sp),
            out_shape=pltpu.VMEM((rows, model), BF16),
            in_specs=[hbm()] * 6,
            out_specs=vmem(),
            scratch_shapes=[
                pltpu.VMEM((1, model), F32),
                pltpu.VMEM((w_out.shape[0], half), BF16),
                pltpu.VMEM((model, units), BF16),
                pltpu.VMEM((units // 2, half), BF16),
                pltpu.VMEM((units // 2, half), BF16),
                pltpu.VMEM((chip_rows, half), F32),
                pltpu.VMEM((n_sp, per_share + 1, heads, head_dim), F32),
                pltpu.VMEM((chip_rows * heads, head_dim), F32),
                pltpu.VMEM((OUT_CHUNKS, n_tp, chip_rows, half // OUT_CHUNKS), F32),
                pltpu.VMEM((2, chip_rows, half), F32),
                pltpu.VMEM((chip_rows, model), BF16),
                pltpu.VMEM((DOWN_CHUNKS, chip_rows, half // DOWN_CHUNKS), F32),
                pltpu.VMEM((DOWN_CHUNKS, chip_rows, half // DOWN_CHUNKS), F32),
                pltpu.VMEM((DOWN_CHUNKS, n_tp, chip_rows, half // DOWN_CHUNKS), F32),
                pltpu.VMEM((DOWN_CHUNKS, n_sp, chip_rows, half // DOWN_CHUNKS), F32),
                dma((6 + 2 * GU_SPLITS,)),
                dma((n_sp - 1,)), dma((n_sp - 1,)),
                dma((1 + OUT_CHUNKS + DOWN_CHUNKS,)), dma((1 + OUT_CHUNKS + DOWN_CHUNKS,)),
                dma((OUT_CHUNKS, n_tp - 1)), dma((OUT_CHUNKS, n_tp - 1)),
                dma((DOWN_CHUNKS, n_tp - 1)), dma((DOWN_CHUNKS, n_tp - 1)),
                dma((DOWN_CHUNKS, n_sp - 1)), dma((DOWN_CHUNKS, n_sp - 1)),
            ],
            compiler_params=pltpu.CompilerParams(vmem_limit_bytes=TAIL_VMEM, collective_id=0, has_side_effects=True),
            name='tail',
        )(parts, resid, norm_mlp[None, :], w_out, w_gate_up, w_down)
        return result, k_upd.reshape(k_cache.shape), v_upd.reshape(v_cache.shape)

    return jax.shard_map(local_step, mesh=mesh, in_specs=(P('dp', None), P('dp'), P(None), P(None), P(None, 'tp'), P('tp', None), P(None, 'tp'), P('tp', None), cache_spec, cache_spec), out_specs=(P('dp', None), cache_spec, cache_spec), check_vma=False)
```

```python
import functools

import jax
import jax.numpy as jnp
import numpy as np
from jax import lax
from jax.experimental import pallas as pl
from jax.experimental.pallas import tpu as pltpu
from jax.sharding import PartitionSpec as P

WINDOW = 2047
ROPE_BASE = 10000.0
NORM_EPS = 1e-5
MESH = pl.DeviceIdType.MESH
LANES = 128
QKV_CHUNKS = 4
OUT_CHUNKS = 2
DOWN_CHUNKS = 2
GU_SPLITS = 1
ATTEND_VMEM = 60 * 1024 * 1024
TAIL_VMEM = 52 * 1024 * 1024
F32, BF16 = jnp.float32, jnp.bfloat16


def dot(lhs, rhs):
    return jnp.dot(lhs, rhs, preferred_element_type=F32)


def dot_t(lhs, rhs):
    return lax.dot_general(lhs, rhs, (((1,), (1,)), ((), ())), preferred_element_type=F32)


def round_bf16(values):
    return values.astype(BF16).astype(F32)


def row_scale(values):
    return lax.rsqrt(jnp.mean(values * values, axis=-1, keepdims=True) + NORM_EPS)


def attend_kernel(dims, pos_hbm, hid_hbm, gain_hbm, freq_hbm, w_hbm, k_hbm, v_hbm, ko_hbm, vo_hbm, part_hbm, resid_hbm,
                  pos_ref, hid_ref, gain_ref, freq_ref, w_buf, k_buf, v_buf, norm_buf, proj_buf, q_buf, new_buf, s_buf,
                  part_ref, resid_ref, in_sem, w_sem, k_sem, v_sem, ko_sem, vo_sem, out_sem):
    rows, block_len, kv_count, group, shares = dims
    heads = kv_count * group
    per_share = rows // shares
    w_rows = w_buf.shape[0] // QKV_CHUNKS

    def w_copy(c):
        part = pl.ds(c * w_rows, w_rows)
        return pltpu.make_async_copy(w_hbm.at[part], w_buf.at[part], w_sem.at[c])

    def cache_copy(src, dst, sem, g):
        part = pl.ds(g * per_share, per_share)
        return pltpu.make_async_copy(src.at[part], dst.at[part], sem.at[g])

    small = [pltpu.make_async_copy(src, dst, in_sem.at[n]) for n, (src, dst) in enumerate(
        [(hid_hbm, hid_ref), (gain_hbm, gain_ref), (freq_hbm, freq_ref), (pos_hbm, pos_ref)])]
    for copy in small:
        copy.start()
    for c in range(QKV_CHUNKS):
        w_copy(c).start()
    for g in range(shares):
        cache_copy(k_hbm, k_buf, k_sem, g).start()
    for copy in small:
        copy.wait()

    resid = hid_ref[...].astype(F32)
    for n in range(resid_ref.shape[0]):
        resid_ref[n] = resid[n * 2 * per_share:(n + 1) * 2 * per_share]
    resid_copy = pltpu.make_async_copy(resid_ref, resid_hbm, out_sem.at[0])
    resid_copy.start()
    norm_buf[...] = (resid * row_scale(resid) * gain_ref[...]).astype(BF16)

    row_id = lax.broadcasted_iota(jnp.int32, (8, LANES), 0)
    tiles = []
    for r in range(rows // 8):
        tile = jnp.zeros((8, LANES), jnp.int32)
        for i in range(8):
            tile = jnp.where(row_id == i, pos_ref[r * 8 + i], tile)
        tiles.append(tile)
    angles = jnp.concatenate(tiles, axis=0).astype(F32) * freq_ref[...]
    cos_tab = jnp.cos(angles)
    sin_tab = jnp.sin(angles)
    lane_id = lax.broadcasted_iota(jnp.int32, (rows, LANES), 1)
    sin_tab = jnp.where(lane_id < LANES // 2, -sin_tab, sin_tab)

    def rope(values):
        return values * cos_tab + pltpu.roll(values, LANES // 2, axis=1) * sin_tab

    for c in range(QKV_CHUNKS):
        part = slice(c * w_rows, (c + 1) * w_rows)
        w_copy(c).wait()
        if c == QKV_CHUNKS - 1:
            for g in range(shares):
                cache_copy(v_hbm, v_buf, v_sem, g).start()
        term = dot(norm_buf[:, part], w_buf[part, :])
        proj_buf[...] = term if c == 0 else proj_buf[...] + term

    for kv in range(kv_count):
        base = kv * (group + 2) * LANES
        for g in range(group):
            q_new = round_bf16(rope(proj_buf[:, base + g * LANES:base + (g + 1) * LANES]))
            q_buf[pl.ds(kv * group + g, rows, stride=heads), :] = q_new
        k_col = base + group * LANES
        new_buf[pl.ds(kv, rows, stride=8), :] = round_bf16(rope(proj_buf[:, k_col:k_col + LANES]))
        new_buf[pl.ds(kv_count + kv, rows, stride=8), :] = round_bf16(proj_buf[:, k_col + LANES:k_col + 2 * LANES])

    start = lax.axis_index('sp') * block_len
    score_scale = LANES ** -0.5
    tile_rows = 8 * kv_count
    tile_id = lax.broadcasted_iota(jnp.int32, (tile_rows, LANES), 0)
    col_id = lax.broadcasted_iota(jnp.int32, (heads, block_len * kv_count), 1)
    head_id = lax.broadcasted_iota(jnp.int32, (heads, block_len * kv_count), 0)
    own_kv = lax.rem(col_id, kv_count) == head_id // group
    slot_id = jnp.where(own_kv, start + col_id // kv_count, -1)
    stat_lane = lax.broadcasted_iota(jnp.int32, (heads, LANES), 1)

    def write_row(buf, b, first):
        slot = pos_ref[b] - start

        @pl.when(jnp.logical_and(slot >= 0, slot < block_len))
        def _():
            base = pl.multiple_of((slot // 8) * tile_rows, tile_rows)
            tile = buf[b, pl.ds(base, tile_rows), :].astype(F32)
            lines = new_buf[pl.ds(pl.multiple_of(b * 8, 8), 8), :]
            new = jnp.zeros((tile_rows, LANES), F32)
            for kv in range(kv_count):
                line = lines[first + kv:first + kv + 1, :]
                new = jnp.where(lax.rem(tile_id, kv_count) == kv, line, new)
            hit = tile_id // kv_count == lax.rem(slot, 8)
            buf[b, pl.ds(base, tile_rows), :] = jnp.where(hit, new, tile).astype(BF16)

    def key_step(g, carry):
        cache_copy(k_hbm, k_buf, k_sem, g).wait()
        for i in range(per_share):
            write_row(k_buf, g * per_share + i, 0)
        cache_copy(k_buf, ko_hbm, ko_sem, g).start()
        for i in range(per_share):
            b = g * per_share + i
            q_rows = q_buf[pl.ds(pl.multiple_of(b * heads, heads), heads), :].astype(BF16)
            s_buf[b] = dot_t(q_rows, k_buf[b])
        return carry

    def weight_step(g, carry):
        stats = jnp.zeros((heads, LANES), F32)
        for i in range(per_share):
            b = g * per_share + i
            pos = pos_ref[b]
            seen = (slot_id <= pos) & (slot_id >= jnp.maximum(pos - WINDOW, 0))
            scores = jnp.where(seen, s_buf[b] * score_scale, -jnp.inf)
            top = jnp.max(scores, axis=-1, keepdims=True)
            base = jnp.where(top == -jnp.inf, 0.0, top)
            weights = jnp.exp(scores - base)
            total = jnp.sum(weights, axis=-1, keepdims=True)
            s_buf[b] = weights
            stats = jnp.where(stat_lane == i, top, stats)
            stats = jnp.where(stat_lane == per_share + i, total, stats)
        part_ref[g, per_share] = stats
        return carry

    def value_step(g, carry):
        cache_copy(v_hbm, v_buf, v_sem, g).wait()
        for i in range(per_share):
            write_row(v_buf, g * per_share + i, kv_count)
        cache_copy(v_buf, vo_hbm, vo_sem, g).start()
        for i in range(per_share):
            b = g * per_share + i
            part_ref[g, i] = dot(s_buf[b].astype(BF16), v_buf[b])
        return carry

    lax.fori_loop(0, shares, key_step, 0)
    lax.fori_loop(0, shares, weight_step, 0)
    lax.fori_loop(0, shares, value_step, 0)
    part_copy = pltpu.make_async_copy(part_ref, part_hbm, out_sem.at[1])
    part_copy.start()
    for g in range(shares):
        cache_copy(k_buf, ko_hbm, ko_sem, g).wait()
        cache_copy(v_buf, vo_hbm, vo_sem, g).wait()
    resid_copy.wait()
    part_copy.wait()


def tail_kernel(n_tp, n_sp, part_hbm, resid_hbm, gain_hbm, wo_hbm, wgu_hbm, wd_hbm, out_ref,
                gain_ref, wo_buf, wgu_buf, wd_own, wd_mate, resid_buf, part_in, att_buf, y1_buf, x1_own, r2_buf,
                z_out, z_in, y2_buf, x2_in, w_sem, b_send, b_recv, m_send, m_recv, y1_send, y1_recv,
                y2_send, y2_recv, g2_send, g2_recv):
    t = lax.axis_index('tp')
    s = lax.axis_index('sp')
    n_chip = n_sp // 2
    chip, core = s // 2, lax.rem(s, 2)
    other = 1 - core
    mate = chip * 2 + other
    units, model = wd_hbm.shape
    core_units = units // 2
    split = core_units // GU_SPLITS
    half = model // 2
    width = half // OUT_CHUNKS
    down_width = half // DOWN_CHUNKS
    per_share = part_hbm.shape[1] - 1
    heads = part_hbm.shape[2]
    share_rows = per_share * heads
    rows = 2 * per_share

    def columns(which, size):
        return pl.ds(pl.multiple_of(which * size, LANES), size)

    resid_load = pltpu.make_async_copy(resid_hbm.at[chip, :, columns(core, half)], resid_buf, w_sem.at[0])
    wo_load = pltpu.make_async_copy(wo_hbm.at[:, columns(core, half)], wo_buf, w_sem.at[1])
    gu_loads = []
    for n in range(GU_SPLITS):
        for side in range(2):
            col = pl.multiple_of(side * units + core * core_units + n * split, LANES)
            at = (2 * n + side) * split
            gu_loads.append(pltpu.make_async_copy(wgu_hbm.at[:, pl.ds(col, split)], wgu_buf.at[:, pl.ds(at, split)], w_sem.at[4 + len(gu_loads)]))
    wd_rows = columns(core, core_units)
    wd_loads = [
        pltpu.make_async_copy(wd_hbm.at[wd_rows, columns(other, half)], wd_mate, w_sem.at[2]),
        pltpu.make_async_copy(wd_hbm.at[wd_rows, columns(core, half)], wd_own, w_sem.at[3]),
    ]
    part_load = pltpu.make_async_copy(part_hbm.at[s], part_in.at[s], w_sem.at[4 + 2 * GU_SPLITS])
    gain_load = pltpu.make_async_copy(gain_hbm, gain_ref, w_sem.at[5 + 2 * GU_SPLITS])
    part_load.start()

    def wrap(value, count):
        return lax.rem(value + count, count)

    barrier = pltpu.get_barrier_semaphore()
    for k in range(1, n_sp):
        pl.semaphore_signal(barrier, inc=1, device_id={'sp': wrap(s + k, n_sp)}, device_id_type=MESH)
    for k in range(1, n_tp):
        pl.semaphore_signal(barrier, inc=1, device_id={'tp': wrap(t + k, n_tp)}, device_id_type=MESH)
    resid_load.start()
    gain_load.start()
    pl.semaphore_wait(barrier, n_sp + n_tp - 2)

    sent = []

    def push(src, dst, send, recv, device):
        copy = pltpu.make_async_remote_copy(src_ref=src, dst_ref=dst, send_sem=send, recv_sem=recv, device_id=device, device_id_type=MESH)
        copy.start()
        sent.append(copy)

    def arrive(dst, recv):
        pltpu.make_async_remote_copy(src_ref=dst, dst_ref=dst, send_sem=b_send.at[0], recv_sem=recv, device_id={'sp': mate}, device_id_type=MESH).wait_recv()

    to_mate = {'sp': mate}
    near_first = sorted(range(1, n_chip), key=lambda k: min(k, n_chip - k))
    far_first = near_first[::-1]

    links = [(k, c) for k in far_first + [0] for c in range(2) if k or c]
    for n, (k, c) in enumerate(links):
        dev = wrap(chip + k, n_chip) * 2 + lax.rem(core + c, 2)
        push(part_hbm.at[dev], part_in.at[s], b_send.at[n], b_recv.at[n], {'sp': dev})
    wo_load.start()
    for load in gu_loads[:2]:
        load.start()
    part_load.wait()
    resid_load.wait()
    gain_load.wait()
    wo_load.wait()
    for n, (k, c) in enumerate(links):
        arrive(part_in.at[wrap(chip - k, n_chip) * 2 + lax.rem(core + c, 2)], b_recv.at[n])
    for load in gu_loads[2:]:
        load.start()
    stats = [part_in[j, per_share] for j in range(n_sp)]
    top = functools.reduce(jnp.maximum, stats)
    scales = [jnp.exp(st - top) for st in stats]
    total = sum(sc * pltpu.roll(st, LANES - per_share, axis=1) for sc, st in zip(scales, stats))
    for i in range(per_share):
        acc = sum(part_in[j, i] * scales[j][:, i:i + 1] for j in range(n_sp))
        at = pl.multiple_of(core * share_rows + i * heads, heads)
        att_buf[pl.ds(at, heads), :] = round_bf16(acc / total[:, i:i + 1])
    mine = att_buf.at[pl.ds(pl.multiple_of(core * share_rows, heads), share_rows)]
    push(mine, mine, m_send.at[0], m_recv.at[0], to_mate)
    arrive(att_buf.at[pl.ds(pl.multiple_of(other * share_rows, heads), share_rows)], m_recv.at[0])
    attended = jnp.concatenate([att_buf[pl.ds(h, rows, stride=heads), :] for h in range(heads)], axis=1).astype(BF16)

    for load in wd_loads:
        load.start()
    for n in range(OUT_CHUNKS):
        y1_buf[n, t] = round_bf16(dot(attended, wo_buf[:, n * width:(n + 1) * width]))
        for k in sorted(range(1, n_tp), key=lambda k: -min(k, n_tp - k)):
            push(y1_buf.at[n, t], y1_buf.at[n, t], y1_send.at[n, k - 1], y1_recv.at[n, k - 1], {'tp': wrap(t + k, n_tp)})
    for n in range(OUT_CHUNKS):
        for k in range(1, n_tp):
            arrive(y1_buf.at[n, wrap(t - k, n_tp)], y1_recv.at[n, k - 1])
        out_sum = functools.reduce(jnp.add, [y1_buf[n, j] for j in range(n_tp)])
        x1_own[core, :, n * width:(n + 1) * width] = resid_buf[:, n * width:(n + 1) * width] + out_sum
        part = x1_own.at[core, :, pl.ds(n * width, width)]
        push(part, part, m_send.at[1 + n], m_recv.at[1 + n], to_mate)
    square = jnp.zeros((rows, LANES), F32)
    for n in range(OUT_CHUNKS):
        arrive(x1_own.at[other, :, pl.ds(n * width, width)], m_recv.at[1 + n])
        for c in range(2):
            for at in range(0, width, LANES):
                piece = x1_own[c, :, n * width + at:n * width + at + LANES]
                square = square + piece * piece
    scale = lax.rsqrt(jnp.sum(square, axis=-1, keepdims=True) / model + NORM_EPS)
    for c in range(2):
        for n in range(OUT_CHUNKS):
            part = slice(c * half + n * width, c * half + (n + 1) * width)
            r2_buf[:, part] = (x1_own[c, :, n * width:(n + 1) * width] * scale * gain_ref[:, part]).astype(BF16)

    acts = []
    for n in range(GU_SPLITS):
        gu_loads[2 * n].wait()
        gu_loads[2 * n + 1].wait()
        both = dot(r2_buf[...], wgu_buf[:, 2 * n * split:2 * (n + 1) * split])
        gate = both[:, :split]
        acts.append((gate * jax.nn.sigmoid(gate) * both[:, split:]).astype(BF16))
    act = jnp.concatenate(acts, axis=1)
    wd_loads[0].wait()
    given = dot(act, wd_mate[...])
    for n in range(DOWN_CHUNKS):
        z_out[n] = given[:, n * down_width:(n + 1) * down_width]
        push(z_out.at[n], z_in.at[n], m_send.at[1 + OUT_CHUNKS + n], m_recv.at[1 + OUT_CHUNKS + n], to_mate)
    wd_loads[1].wait()
    for n in range(DOWN_CHUNKS):
        own = dot(act, wd_own[:, n * down_width:(n + 1) * down_width])
        arrive(z_in.at[n], m_recv.at[1 + OUT_CHUNKS + n])
        y2_buf[n, t] = round_bf16(own + z_in[n])
        for k in sorted(range(1, n_tp), key=lambda k: -min(k, n_tp - k)):
            push(y2_buf.at[n, t], y2_buf.at[n, t], y2_send.at[n, k - 1], y2_recv.at[n, k - 1], {'tp': wrap(t + k, n_tp)})
    for n in range(DOWN_CHUNKS):
        for k in range(1, n_tp):
            arrive(y2_buf.at[n, wrap(t - k, n_tp)], y2_recv.at[n, k - 1])
        down_sum = functools.reduce(jnp.add, [y2_buf[n, j] for j in range(n_tp)])
        x2_in[n, s] = x1_own[core, :, n * down_width:(n + 1) * down_width] + down_sum
        for k in far_first:
            push(x2_in.at[n, s], x2_in.at[n, s], g2_send.at[n, k], g2_recv.at[n, k], {'sp': wrap(chip + k, n_chip) * 2 + core})
        push(x2_in.at[n, s], x2_in.at[n, s], g2_send.at[n, 0], g2_recv.at[n, 0], to_mate)
    for n in range(DOWN_CHUNKS):
        for k in near_first:
            far = x2_in.at[n, wrap(chip - k, n_chip) * 2 + core]
            arrive(far, g2_recv.at[n, k])
            push(far, far, g2_send.at[n, n_chip + k - 1], g2_recv.at[n, n_chip + k - 1], to_mate)
    for n in range(DOWN_CHUNKS):
        arrive(x2_in.at[n, mate], g2_recv.at[n, 0])
        for k in near_first:
            arrive(x2_in.at[n, wrap(chip - k, n_chip) * 2 + other], g2_recv.at[n, n_chip + k - 1])
        for j in range(0, n_chip, 2):
            for c in range(2):
                lines = jnp.concatenate([x2_in[n, 2 * j + c], x2_in[n, 2 * j + 2 + c]], axis=0)
                col = c * half + n * down_width
                out_ref[j * rows:(j + 2) * rows, col:col + down_width] = lines.astype(BF16)
    for copy in sent:
        copy.wait_send()


def vmem():
    return pl.BlockSpec(memory_space=pltpu.VMEM)


def hbm():
    return pl.BlockSpec(memory_space=pl.ANY)


def solution(mesh):
    n_tp, n_sp = mesh.shape['tp'], mesh.shape['sp']
    cache_spec = P('dp', 'sp', 'tp', None)

    def local_step(hidden, positions, norm_attn, norm_mlp, w_qkv, w_out, w_gate_up, w_down, k_cache, v_cache):
        rows, block_len, kv_count, head_dim = k_cache.shape
        model = hidden.shape[1]
        group = w_qkv.shape[1] // (kv_count * head_dim) - 2
        heads = kv_count * group
        shares = n_sp
        per_share = rows // shares
        flat = (rows, block_len * kv_count, head_dim)
        inv_freq = ROPE_BASE ** (-np.arange(0, head_dim, 2) / head_dim)
        freq = jnp.asarray(np.concatenate([inv_freq, inv_freq])[None, :], F32)
        dma = pltpu.SemaphoreType.DMA

        k_upd, v_upd, parts, resid = pl.pallas_call(
            functools.partial(attend_kernel, (rows, block_len, kv_count, group, shares)),
            out_shape=(
                jax.ShapeDtypeStruct(flat, BF16),
                jax.ShapeDtypeStruct(flat, BF16),
                pltpu.VMEM((shares, per_share + 1, heads, head_dim), F32),
                pltpu.VMEM((shares // 2, 2 * per_share, model), F32),
            ),
            in_specs=[hbm()] * 7,
            out_specs=(hbm(), hbm(), hbm(), hbm()),
            scratch_shapes=[
                pltpu.SMEM(positions.shape, jnp.int32),
                pltpu.VMEM(hidden.shape, BF16),
                pltpu.VMEM((1, model), F32),
                pltpu.VMEM(freq.shape, F32),
                pltpu.VMEM(w_qkv.shape, BF16),
                pltpu.VMEM(flat, BF16),
                pltpu.VMEM(flat, BF16),
                pltpu.VMEM((rows, model), BF16),
                pltpu.VMEM((rows, w_qkv.shape[1]), F32),
                pltpu.VMEM((rows * heads, head_dim), F32),
                pltpu.VMEM((rows * 8, head_dim), F32),
                pltpu.VMEM((rows, heads, block_len * kv_count), F32),
                pltpu.VMEM((shares, per_share + 1, heads, head_dim), F32),
                pltpu.VMEM((shares // 2, 2 * per_share, model), F32),
                dma((4,)), dma((QKV_CHUNKS,)), dma((shares,)), dma((shares,)), dma((shares,)), dma((shares,)), dma((2,)),
            ],
            compiler_params=pltpu.CompilerParams(vmem_limit_bytes=ATTEND_VMEM),
            name='attend',
        )(positions, hidden, norm_attn[None, :], freq, w_qkv, k_cache.reshape(flat), v_cache.reshape(flat))

        units = w_down.shape[0]
        chip_rows, half = 2 * per_share, model // 2
        result = pl.pallas_call(
            functools.partial(tail_kernel, n_tp, n_sp),
            out_shape=pltpu.VMEM((rows, model), BF16),
            in_specs=[hbm()] * 6,
            out_specs=vmem(),
            scratch_shapes=[
                pltpu.VMEM((1, model), F32),
                pltpu.VMEM((w_out.shape[0], half), BF16),
                pltpu.VMEM((model, units), BF16),
                pltpu.VMEM((units // 2, half), BF16),
                pltpu.VMEM((units // 2, half), BF16),
                pltpu.VMEM((chip_rows, half), F32),
                pltpu.VMEM((n_sp, per_share + 1, heads, head_dim), F32),
                pltpu.VMEM((chip_rows * heads, head_dim), F32),
                pltpu.VMEM((OUT_CHUNKS, n_tp, chip_rows, half // OUT_CHUNKS), F32),
                pltpu.VMEM((2, chip_rows, half), F32),
                pltpu.VMEM((chip_rows, model), BF16),
                pltpu.VMEM((DOWN_CHUNKS, chip_rows, half // DOWN_CHUNKS), F32),
                pltpu.VMEM((DOWN_CHUNKS, chip_rows, half // DOWN_CHUNKS), F32),
                pltpu.VMEM((DOWN_CHUNKS, n_tp, chip_rows, half // DOWN_CHUNKS), F32),
                pltpu.VMEM((DOWN_CHUNKS, n_sp, chip_rows, half // DOWN_CHUNKS), F32),
                dma((6 + 2 * GU_SPLITS,)),
                dma((n_sp - 1,)), dma((n_sp - 1,)),
                dma((1 + OUT_CHUNKS + DOWN_CHUNKS,)), dma((1 + OUT_CHUNKS + DOWN_CHUNKS,)),
                dma((OUT_CHUNKS, n_tp - 1)), dma((OUT_CHUNKS, n_tp - 1)),
                dma((DOWN_CHUNKS, n_tp - 1)), dma((DOWN_CHUNKS, n_tp - 1)),
                dma((DOWN_CHUNKS, n_sp - 1)), dma((DOWN_CHUNKS, n_sp - 1)),
            ],
            compiler_params=pltpu.CompilerParams(vmem_limit_bytes=TAIL_VMEM, collective_id=0, has_side_effects=True),
            name='tail',
        )(parts, resid, norm_mlp[None, :], w_out, w_gate_up, w_down)
        return result, k_upd.reshape(k_cache.shape), v_upd.reshape(v_cache.shape)

    return jax.shard_map(local_step, mesh=mesh, in_specs=(P('dp', None), P('dp'), P(None), P(None), P(None, 'tp'), P('tp', None), P(None, 'tp'), P('tp', None), cache_spec, cache_spec), out_specs=(P('dp', None), cache_spec, cache_spec), check_vma=False)
```
